512 devices in a mesh: rows: 128 (over x, z, core), rep: 4 (over y).
Axes of the slice: x: 4, y: 4, z: 16, core: 2. Of those that a mesh axis runs over, the one named last changes fastest.
Arguments:
- requests: int32 [512, 128, 8], P(('rows', 'rep')), may hold values from 0 to 1023
- request_counts: int32 [512, 128], P(('rows', 'rep')), may hold values from 0 to 8, as said below
- table: bfloat16 [131072, 512], P('rows')
- gain: float32 [512], replicated, may hold values from 0.5 to 1.5
Outputs:
- normalized: bfloat16 [512, 128, 8, 512], P(('rows', 'rep'))
- row_counts: int32 [131072], P('rows')
- moments: float32 [2, 2], replicated
The draws below stay inside these ranges and needn't reach their ends.
Inputs may be any that keep to these rules, and one draw needn't show every extreme that they name: Each device uses request_counts[d, o] of its 8 slots toward owner o; in every draw one owner's slots are full from every device.
All inputs are finite; a program needn't handle non-finite values.
Results may differ from the reference program's by a relative error of at most 0.0004.
Values may be sent and summed in bfloat16 or wider, within the bound.
A program may use at most 64 MiB of HBM per device.

```python
import math
import jax
import jax.numpy as jnp
import numpy as np
from jax import lax

WIDTH = 256
LAYERS = 2
ROWS_DEV = 1024
VOCAB = 131072
CAP = 8
N_ROWS = 128
DEVICES = 512


def draw_request_counts(key, part):
    first, second, third, fourth = jax.random.split(jax.random.fold_in(key, 11), 4)
    level = jax.random.randint(first, (1, N_ROWS), CAP // 2, CAP + 1)
    hottest = jax.random.randint(second, (), 0, N_ROWS)
    bits_one = jax.random.randint(third, (DEVICES, N_ROWS), 0, 1048576)
    bits_two = jax.random.randint(fourth, (DEVICES, N_ROWS), 0, 1048576)
    picked = jnp.maximum(bits_one % (level + 1), bits_two % (level + 1))
    full_owner = jnp.arange(N_ROWS)[None, :] == hottest
    return jnp.where(full_owner, CAP, picked).astype(jnp.int32)


def draw_table(key, part):
    first, second, third = jax.random.split(jax.random.fold_in(key, 23), 3)
    position = jnp.arange(VOCAB, dtype=jnp.float32) / VOCAB
    row_scale = jnp.exp(jax.random.uniform(second, (VOCAB, 1), jnp.float32, 0.0, math.log(10.0)))
    row_scale = row_scale * (1.0 + 2.0 * position)[:, None]
    col_scale = jnp.exp(jax.random.uniform(third, (1, LAYERS * WIDTH), jnp.float32, math.log(0.5), math.log(2.0)))
    values = jax.random.normal(first, (VOCAB, LAYERS * WIDTH), jnp.float32) * row_scale * col_scale
    return values.astype(jnp.bfloat16)


def set_ends(values, key, low, largest):
    shape = values.shape
    place = [jax.random.randint(jax.random.fold_in(key, axis), (), 0, shape[axis]) for axis in range(len(shape))]
    values = values.at[tuple(place)].set(low)
    longest = shape.index(max(shape))
    place[longest] = (place[longest] + 1) % shape[longest]
    return values.at[tuple(place)].set(largest)


def rank_bounds(count, slope):
    portions = [(1 << 20) // math.isqrt(standing ** slope) + 1 for standing in range(1, count + 1)]
    spread = 1 + sum(portions) // (1 << 30)
    return np.cumsum(np.array([max(1, weight // spread) for weight in portions]))


def ranked_ids(key, shape, count, skew):
    grid = rank_bounds(count, skew)
    lot = jax.random.randint(jax.random.fold_in(key, 1), shape, 0, int(grid[count - 1]))
    rank = jnp.searchsorted(jnp.asarray(grid, jnp.int32), lot, side="right")
    return jax.random.permutation(jax.random.fold_in(key, 2), count)[rank].astype(jnp.int32)


def setup_inputs(seed: int = 0) -> dict:
    key_list = jax.random.split(jax.random.key(seed), 5)
    requests = set_ends(ranked_ids(key_list[0], (DEVICES, N_ROWS, CAP), ROWS_DEV, 2), jax.random.fold_in(key_list[0], 3), 0, ROWS_DEV - 1).astype(jnp.int32)
    request_counts = draw_request_counts(jax.random.fold_in(key_list[4], 71), 0)
    table = draw_table(jax.random.fold_in(key_list[4], 71), 0)
    gain = jnp.clip(1.0 + 0.1 * jax.random.normal(key_list[3], (LAYERS * WIDTH,), jnp.float32), 0.5, 1.5)
    return dict(requests=requests, request_counts=request_counts, table=table, gain=gain)


epsilon = 1e-06

def reference(requests, request_counts, table, gain):
    offsets = (jnp.arange(N_ROWS, dtype=jnp.int32) * ROWS_DEV)[None, :, None]
    global_index = (requests + offsets).astype(jnp.int32)
    slot_index = jnp.arange(CAP, dtype=jnp.int32)[None, None, :]
    live_slot = slot_index < request_counts[:, :, None]
    row_counts = jnp.zeros((VOCAB,), jnp.int32).at[global_index.reshape(-1)].add(live_slot.reshape(-1).astype(jnp.int32))
    shaped = table.astype(jnp.float32).reshape(VOCAB, LAYERS, WIDTH)
    weights = row_counts.astype(jnp.float32)
    entries = jnp.sum(weights) * WIDTH
    layer_mean = jnp.dot(weights, lax.optimization_barrier(jnp.sum(shaped, axis=2)), precision=lax.Precision.HIGHEST) / entries
    centered = lax.optimization_barrier(jnp.sum(jnp.square(shaped - layer_mean[None, :, None]), axis=2))
    layer_var = jnp.dot(weights, centered, precision=lax.Precision.HIGHEST) / entries
    inverse = jnp.repeat(lax.rsqrt(layer_var + epsilon), WIDTH) * gain
    mean_full = jnp.repeat(layer_mean, WIDTH)

    def one_device(pair):
        index_rows, live_rows = pair
        fetched = jnp.take(table, index_rows.reshape(-1), axis=0).astype(jnp.float32)
        scaled = (fetched - mean_full) * inverse
        scaled = jnp.where(live_rows.reshape(-1, 1), scaled, jnp.zeros_like(scaled))
        return scaled.reshape(N_ROWS, CAP, LAYERS * WIDTH).astype(jnp.bfloat16)
    normalized = lax.map(one_device, (global_index, live_slot))
    return (normalized, row_counts, jnp.stack([layer_mean, layer_var]))
```

```python
import functools

import jax
import jax.numpy as jnp
from jax import lax
from jax.experimental import pallas as pl
from jax.experimental.pallas import tpu as pltpu
from jax.sharding import Mesh
from jax.sharding import PartitionSpec as P

WIDTH = 256
LAYERS = 2
LANES = 128
ROWS = ("rows_0", "rows_1", "rows_2")
ROWS_REP = ("rows_0", "rows_1", "rows_2", "rep")
MESH = pl.DeviceIdType.MESH

epsilon = 1e-06


def merged(parts, lane):
    def pick(at):
        found = jnp.sum(jnp.where(lane == at, parts, 0.0), axis=2, keepdims=True)
        return jnp.broadcast_to(found, parts.shape)

    def over(value):
        return jnp.sum(value, axis=0, keepdims=True)

    line = lane[:1]
    each = pick(0)
    entries = over(each)
    row = jnp.where(line == 0, entries, 0.0)
    for layer in range(LAYERS):
        mean_each = pick(1 + layer)
        mean = over(each * mean_each) / jnp.maximum(entries, 1.0)
        gap = mean_each - mean
        square = over(pick(1 + LAYERS + layer) + each * gap * gap)
        row = jnp.where(line == 1 + layer, mean, row)
        row = jnp.where(line == 1 + LAYERS + layer, square, row)
    return row


def exchange(
    sizes,
    slots,
    ids_ref,
    table_ref,
    rows_ref,
    counts_ref,
    moments_ref,
    table,
    heard,
    asked,
    column,
    packed,
    passing,
    totals,
    tally,
    tally_all,
    own_row,
    side_row,
    plane_row,
    parts_rep,
    parts_side,
    parts_ring,
    local_sem,
    ids_send,
    ids_recv,
    ids_keep,
    ask_send,
    ask_recv,
    row_send,
    row_recv,
    out_send,
    out_recv,
    out_keep,
    tally_send,
    tally_recv,
    rep_send,
    rep_recv,
    side_send,
    side_recv,
    ring_send,
    ring_recv,
):
    count_x, count_z, count_c, count_y = sizes
    count_s = count_x * count_c
    held = table.shape[0]
    width = table.shape[1]
    x = lax.axis_index("rows_0")
    z = lax.axis_index("rows_1")
    c = lax.axis_index("rows_2")
    y = lax.axis_index("rep")
    side = x * count_c + c

    def on_ring(at):
        return {"rows_1": at}

    def on_side(at):
        return {"rows_0": lax.div(at, count_c), "rows_2": lax.rem(at, count_c)}

    def on_rep(at):
        return {"rep": at}

    ring_peers = [lax.rem(z + k, count_z) for k in range(1, count_z)]
    side_peers = [lax.rem(side + k, count_s) for k in range(1, count_s)]
    rep_peers = [lax.rem(y + k, count_y) for k in range(1, count_y)]

    def plane(step):
        far = lax.div(step + 1, 2)
        toward = 2 * lax.rem(step, 2) - 1
        return lax.rem(z + far * toward + count_z, count_z)

    load_table = pltpu.make_async_copy(table_ref, table, local_sem.at[0])
    load_table.start()
    load_ids = pltpu.make_async_copy(ids_ref.at[z], heard.at[z], local_sem.at[1])
    load_ids.start()

    barrier = pltpu.get_barrier_semaphore()
    for peer in ring_peers:
        pl.semaphore_signal(barrier, inc=1, device_id=on_ring(peer), device_id_type=MESH)
    for peer in side_peers:
        pl.semaphore_signal(barrier, inc=1, device_id=on_side(peer), device_id_type=MESH)
    for peer in rep_peers:
        pl.semaphore_signal(barrier, inc=1, device_id=on_rep(peer), device_id_type=MESH)
    pl.semaphore_wait(barrier, len(ring_peers) + len(side_peers) + len(rep_peers))

    def ids_copy(at):
        return pltpu.make_async_remote_copy(
            src_ref=ids_ref.at[at],
            dst_ref=heard.at[z],
            send_sem=ids_send.at[at],
            recv_sem=ids_recv.at[z],
            device_id=on_ring(at),
            device_id_type=MESH,
        )

    def ids_arrive(at):
        pltpu.make_async_copy(heard.at[at], heard.at[at], ids_recv.at[at]).wait()

    def start_ids(step, carry):
        ids_copy(plane(step)).start()
        return carry

    lax.fori_loop(1, count_z, start_ids, 0)

    def keep_copy(at):
        return pltpu.make_async_copy(heard.at[at], asked.at[at, side], ids_keep.at[at])

    def tell(at):
        keep_copy(at).start()
        for peer in side_peers:
            pltpu.make_async_remote_copy(
                src_ref=heard.at[at],
                dst_ref=asked.at[at, side],
                send_sem=ask_send.at[at],
                recv_sem=ask_recv.at[at],
                device_id=on_side(peer),
                device_id_type=MESH,
            ).start()

    def hear(step, carry=0):
        at = plane(step)
        ids_arrive(at)
        tell(at)
        return carry

    totals[...] = jnp.zeros_like(totals)
    tally[...] = jnp.zeros_like(tally)

    def look(step, carry=0):
        at = plane(step)
        keep_copy(at).wait()
        several = asked.at[at, pl.ds(0, count_s - 1)]
        pltpu.make_async_copy(several, several, ask_recv.at[at]).wait()
        shape = (count_s, slots, LANES)
        ids = jnp.broadcast_to(asked[at].astype(jnp.float32), shape)
        mine = lax.broadcasted_iota(jnp.int32, shape, 2) == side * slots + lax.broadcasted_iota(
            jnp.int32, shape, 1
        )
        wanted = jnp.sum(jnp.where(mine, ids, 0.0), axis=2, keepdims=True)
        wanted = jnp.broadcast_to(wanted, shape).reshape(count_s * slots, LANES)
        column[at] = wanted
        row_of = lax.broadcasted_iota(jnp.int32, wanted.shape, 1).astype(jnp.float32)
        hot = jnp.concatenate(
            [
                jnp.where(wanted == row_of + float(first), 1.0, 0.0).astype(jnp.bfloat16)
                for first in range(0, held, LANES)
            ],
            axis=1,
        )
        found = jnp.dot(hot, table[...], preferred_element_type=jnp.float32)
        found = found.reshape(count_s, slots, width)
        packed[at] = found.astype(jnp.bfloat16)
        totals[...] += jnp.sum(found, axis=0)
        ones = jnp.ones((8, count_s * slots), jnp.bfloat16)
        tally[...] += jnp.dot(ones, hot, preferred_element_type=jnp.float32)
        return carry

    def row_copy(at):
        return pltpu.make_async_remote_copy(
            src_ref=packed.at[at],
            dst_ref=passing.at[z],
            send_sem=row_send.at[at],
            recv_sem=row_recv.at[z],
            device_id=on_ring(at),
            device_id_type=MESH,
        )

    held_back = min(3, count_z - 1)

    def give(step):
        @pl.when(step >= held_back)
        def _():
            row_copy(plane(step)).start()

    ahead = min(5, count_z - 2)
    load_ids.wait()
    tell(z)
    lax.fori_loop(1, ahead + 1, hear, 0)
    load_table.wait()

    def both(step, carry):
        look(step)
        hear(step + ahead + 1)
        give(step - 1)
        return carry

    def only(step, carry):
        look(step)
        give(step - 1)
        return carry

    lax.fori_loop(0, count_z - 1 - ahead, both, 0)
    lax.fori_loop(count_z - 1 - ahead, count_z, only, 0)

    tally_all[y] = tally[0:1].astype(jnp.int32)
    entries = jnp.sum(tally[0:1], axis=1, keepdims=True) * float(WIDTH)
    summed = jnp.sum(totals[...], axis=0, keepdims=True)
    means = [
        jnp.sum(summed[:, layer * WIDTH : (layer + 1) * WIDTH], axis=1, keepdims=True)
        / jnp.maximum(entries, 1.0)
        for layer in range(LAYERS)
    ]
    center = jnp.concatenate([jnp.broadcast_to(m, (1, WIDTH)) for m in means], axis=1)
    give(count_z - 1)

    def squares(at, total):
        used = column[at] >= 0.0
        used = jnp.concatenate([used.astype(jnp.float32)] * (width // LANES), axis=1)
        used = used.reshape(count_s, slots, width)
        away = (packed[at].astype(jnp.float32) - center[None]) * used
        return total + jnp.sum(away * away, axis=0)

    spread = lax.fori_loop(0, count_z, squares, jnp.zeros((slots, width), jnp.float32))
    spread = jnp.sum(spread, axis=0, keepdims=True)
    lane = lax.broadcasted_iota(jnp.int32, (1, LANES), 1)
    row = jnp.where(lane == 0, entries, 0.0)
    for layer in range(LAYERS):
        square = jnp.sum(spread[:, layer * WIDTH : (layer + 1) * WIDTH], axis=1, keepdims=True)
        row = jnp.where(lane == 1 + layer, means[layer], row)
        row = jnp.where(lane == 1 + LAYERS + layer, square, row)
    own_row[...] = row[None]
    parts_rep[y] = row

    def out_row(at):
        return (x * count_z + at) * count_c + c

    def out_keep_copy(at):
        return pltpu.make_async_copy(
            passing.at[at, side], rows_ref.at[out_row(at)], out_keep.at[at]
        )

    def pass_on(source, at):
        pltpu.make_async_copy(source.at[at, side], rows_ref.at[out_row(at)], out_keep.at[at]).start()
        for peer in side_peers:
            pltpu.make_async_remote_copy(
                src_ref=source.at[at, peer],
                dst_ref=rows_ref.at[out_row(at)],
                send_sem=out_send.at[at],
                recv_sem=out_recv.at[at],
                device_id=on_side(peer),
                device_id_type=MESH,
            ).start()

    def relay(step, carry=0):
        at = plane(step)
        pltpu.make_async_copy(passing.at[at], passing.at[at], row_recv.at[at]).wait()
        pass_on(passing, at)
        return carry

    pass_on(packed, z)

    def tally_copy(peer):
        return pltpu.make_async_remote_copy(
            src_ref=tally_all.at[y],
            dst_ref=tally_all.at[y],
            send_sem=tally_send.at[peer],
            recv_sem=tally_recv.at[y],
            device_id=on_rep(peer),
            device_id_type=MESH,
        )

    def part_copy(source, parts, me, peer, place, send, recv):
        return pltpu.make_async_remote_copy(
            src_ref=source.at[0],
            dst_ref=parts.at[me],
            send_sem=send.at[peer],
            recv_sem=recv.at[me],
            device_id=place(peer),
            device_id_type=MESH,
        )

    def part_arrive(parts, peer, recv):
        pltpu.make_async_copy(parts.at[peer], parts.at[peer], recv.at[peer]).wait()

    def lanes_of(count):
        return lax.broadcasted_iota(jnp.int32, (count, 1, LANES), 2)

    for peer in rep_peers:
        part_copy(own_row, parts_rep, y, peer, on_rep, rep_send, rep_recv).start()
    for peer in rep_peers:
        tally_copy(peer).start()
    for peer in rep_peers:
        part_arrive(parts_rep, peer, rep_recv)
    side_row[...] = merged(parts_rep[...], lanes_of(count_y))
    parts_side[side] = side_row[0]
    for peer in rep_peers:
        pltpu.make_async_copy(tally_all.at[peer], tally_all.at[peer], tally_recv.at[peer]).wait()
    counts_ref[...] = jnp.sum(tally_all[...], axis=0)
    for peer in side_peers:
        part_copy(side_row, parts_side, side, peer, on_side, side_send, side_recv).start()
    for peer in side_peers:
        part_arrive(parts_side, peer, side_recv)
    plane_row[...] = merged(parts_side[...], lanes_of(count_s))
    parts_ring[z] = plane_row[0]
    if held_back < count_z - 1:
        relay(held_back)
    for peer in ring_peers:
        part_copy(plane_row, parts_ring, z, peer, on_ring, ring_send, ring_recv).start()
    for step in range(1, held_back):
        row_copy(plane(step)).start()
    first_rest = held_back + 1 if held_back < count_z - 1 else held_back
    lax.fori_loop(first_rest, count_z, relay, 0)
    for step in range(1, held_back):
        relay(step)
    for peer in ring_peers:
        part_arrive(parts_ring, peer, ring_recv)
    whole = merged(parts_ring[...], lanes_of(count_z))
    moments_ref[...] = whole[0]

    def finish(at, carry):
        several_ids = asked.at[at, pl.ds(0, count_s - 1)]
        pltpu.make_async_copy(several_ids, several_ids, ask_send.at[at]).wait()
        several_rows = rows_ref.at[pl.ds(0, count_s - 1)]
        pltpu.make_async_copy(several_rows, several_rows, out_send.at[at]).wait()
        pltpu.make_async_copy(several_rows, several_rows, out_recv.at[at]).wait()
        out_keep_copy(at).wait()
        return carry

    lax.fori_loop(0, count_z, finish, 0)

    def sent(step, carry):
        at = plane(step)
        ids_copy(at).wait_send()
        row_copy(at).wait_send()
        return carry

    lax.fori_loop(1, count_z, sent, 0)
    for peer in ring_peers:
        part_copy(plane_row, parts_ring, z, peer, on_ring, ring_send, ring_recv).wait_send()
    for peer in side_peers:
        part_copy(side_row, parts_side, side, peer, on_side, side_send, side_recv).wait_send()
    for peer in rep_peers:
        part_copy(own_row, parts_rep, y, peer, on_rep, rep_send, rep_recv).wait_send()
        tally_copy(peer).wait_send()


def per_device(requests, request_counts, table, gain):
    sizes = tuple(lax.axis_size(axis) for axis in ROWS_REP)
    count_x, count_z, count_c, count_y = sizes
    count_s = count_x * count_c
    owners, slots = requests.shape[1:]
    held, width = table.shape
    slot = lax.broadcasted_iota(jnp.int32, (owners, slots), 1)
    live = slot < request_counts[0][:, None]
    ids = jnp.where(live, requests[0], -1).reshape(count_x, count_z, count_c, slots)
    ids = ids.transpose(1, 0, 2, 3).reshape(count_z, 1, count_s * slots)
    ids = jnp.pad(ids, ((0, 0), (0, 0), (0, LANES - count_s * slots)), constant_values=-1)

    dma = pltpu.SemaphoreType.DMA
    vmem = pltpu.VMEM
    rows, tally, moments = pl.pallas_call(
        functools.partial(exchange, sizes, slots),
        out_shape=(
            jax.ShapeDtypeStruct((owners, slots, width), jnp.bfloat16),
            jax.ShapeDtypeStruct((1, held), jnp.int32),
            jax.ShapeDtypeStruct((1, LANES), jnp.float32),
        ),
        in_specs=[
            pl.BlockSpec(memory_space=pltpu.VMEM),
            pl.BlockSpec(memory_space=pl.ANY),
        ],
        out_specs=(
            pl.BlockSpec(memory_space=pl.ANY),
            pl.BlockSpec(memory_space=pltpu.VMEM),
            pl.BlockSpec(memory_space=pltpu.VMEM),
        ),
        scratch_shapes=[
            vmem((held, width), jnp.bfloat16),
            vmem((count_z, 1, LANES), jnp.int32),
            vmem((count_z, count_s, 1, LANES), jnp.int32),
            vmem((count_z, count_s * slots, LANES), jnp.float32),
            vmem((count_z, count_s, slots, width), jnp.bfloat16),
            vmem((count_z, count_s, slots, width), jnp.bfloat16),
            vmem((slots, width), jnp.float32),
            vmem((8, held), jnp.float32),
            vmem((count_y, 1, held), jnp.int32),
            vmem((1, 1, LANES), jnp.float32),
            vmem((1, 1, LANES), jnp.float32),
            vmem((1, 1, LANES), jnp.float32),
            vmem((count_y, 1, LANES), jnp.float32),
            vmem((count_s, 1, LANES), jnp.float32),
            vmem((count_z, 1, LANES), jnp.float32),
            dma((2,)),
            dma((count_z,)),
            dma((count_z,)),
            dma((count_z,)),
            dma((count_z,)),
            dma((count_z,)),
            dma((count_z,)),
            dma((count_z,)),
            dma((count_z,)),
            dma((count_z,)),
            dma((count_z,)),
            dma((count_y,)),
            dma((count_y,)),
            dma((count_y,)),
            dma((count_y,)),
            dma((count_s,)),
            dma((count_s,)),
            dma((count_z,)),
            dma((count_z,)),
        ],
        compiler_params=pltpu.CompilerParams(collective_id=0, has_side_effects=True),
    )(ids, table)

    entries = moments[0, 0]
    layer_mean = moments[0, 1 : 1 + LAYERS]
    layer_var = moments[0, 1 + LAYERS : 1 + 2 * LAYERS] / entries
    inverse = jnp.repeat(lax.rsqrt(layer_var + epsilon), WIDTH) * gain
    finished = (rows.astype(jnp.float32) - jnp.repeat(layer_mean, WIDTH)) * inverse
    normalized = jnp.where(live[..., None], finished, 0.0).astype(jnp.bfloat16)
    return (normalized[None], tally[0], jnp.stack([layer_mean, layer_var]))


def solution(mesh):
    count_y = mesh.shape["rep"]
    cores = 2
    count_x = mesh.devices.shape[0] // (16 * cores)
    finer = Mesh(mesh.devices.reshape(count_x, 16, cores, count_y), ROWS_REP)
    placed = (P(ROWS_REP, None, None), P(ROWS_REP, None), P(ROWS, None), P())
    return jax.shard_map(
        per_device,
        mesh=finer,
        in_specs=placed,
        out_specs=(P(ROWS_REP, None, None, None), P(ROWS), P()),
        check_vma=False,
    )
```

```python
import functools

import jax
import jax.numpy as jnp
from jax import lax
from jax.experimental import pallas as pl
from jax.experimental.pallas import tpu as pltpu
from jax.sharding import Mesh
from jax.sharding import PartitionSpec as P

WIDTH = 256
LAYERS = 2
LANES = 128
ROWS = ("rows_0", "rows_1", "rows_2")
ROWS_REP = ("rows_0", "rows_1", "rows_2", "rep")
MESH = pl.DeviceIdType.MESH

epsilon = 1e-06


def merged(parts, lane):
    def pick(at):
        found = jnp.sum(jnp.where(lane == at, parts, 0.0), axis=2, keepdims=True)
        return jnp.broadcast_to(found, parts.shape)

    def over(value):
        return jnp.sum(value, axis=0, keepdims=True)

    line = lane[:1]
    each = pick(0)
    entries = over(each)
    row = jnp.where(line == 0, entries, 0.0)
    for layer in range(LAYERS):
        mean_each = pick(1 + layer)
        mean = over(each * mean_each) / jnp.maximum(entries, 1.0)
        gap = mean_each - mean
        square = over(pick(1 + LAYERS + layer) + each * gap * gap)
        row = jnp.where(line == 1 + layer, mean, row)
        row = jnp.where(line == 1 + LAYERS + layer, square, row)
    return row


def exchange(
    sizes,
    slots,
    requests_ref,
    used_ref,
    gain_ref,
    table_ref,
    rows_ref,
    counts_ref,
    moments_ref,
    affine_ref,
    table,
    upright,
    ids_ref,
    heard,
    asked,
    column,
    packed,
    passing,
    turned,
    totals,
    tally,
    tally_all,
    own_row,
    side_row,
    plane_row,
    parts_rep,
    parts_side,
    parts_ring,
    local_sem,
    ids_send,
    ids_recv,
    ids_keep,
    ask_send,
    ask_recv,
    row_send,
    row_recv,
    turn_send,
    turn_recv,
    turn_keep,
    out_send,
    out_recv,
    out_keep,
    tally_send,
    tally_recv,
    rep_send,
    rep_recv,
    side_send,
    side_recv,
    ring_send,
    ring_recv,
):
    count_x, count_z, count_c, count_y = sizes
    count_s = count_x * count_c
    held = table.shape[0]
    width = table.shape[1]
    x = lax.axis_index("rows_0")
    z = lax.axis_index("rows_1")
    c = lax.axis_index("rows_2")
    y = lax.axis_index("rep")
    side = x * count_c + c

    def on_ring(at):
        return {"rows_1": at}

    def on_side(at):
        return {"rows_0": lax.div(at, count_c), "rows_2": lax.rem(at, count_c)}

    def on_rep(at):
        return {"rep": at}

    ring_peers = [lax.rem(z + k, count_z) for k in range(1, count_z)]
    side_peers = [lax.rem(side + k, count_s) for k in range(1, count_s)]
    rep_peers = [lax.rem(y + k, count_y) for k in range(1, count_y)]

    def plane(step):
        far = lax.div(step + 1, 2)
        toward = 2 * lax.rem(step, 2) - 1
        return lax.rem(z + far * toward + count_z, count_z)

    load_table = pltpu.make_async_copy(table_ref, table, local_sem.at[0])
    load_table.start()

    barrier = pltpu.get_barrier_semaphore()
    for peer in ring_peers:
        pl.semaphore_signal(barrier, inc=1, device_id=on_ring(peer), device_id_type=MESH)
    for peer in side_peers:
        pl.semaphore_signal(barrier, inc=1, device_id=on_side(peer), device_id_type=MESH)
    for peer in rep_peers:
        pl.semaphore_signal(barrier, inc=1, device_id=on_rep(peer), device_id_type=MESH)

    slot = lax.broadcasted_iota(jnp.int32, requests_ref.shape, 0)
    ids = jnp.where(slot < used_ref[...], requests_ref[...], -1)
    owners = ids.shape[1]
    ids = jnp.concatenate([ids, jnp.zeros((LANES - slots, owners), jnp.int32)], axis=0)
    upright[...] = jnp.transpose(ids)
    lines = jnp.zeros((count_z, LANES), jnp.int32)
    for at in range(count_s):
        first = (at // count_c) * count_z * count_c + at % count_c
        line = upright[pl.ds(first, count_z, stride=count_c), :]
        lines += pltpu.roll(line, slots * at, 1) if at else line
    ids_ref[...] = lines.reshape(count_z, 1, LANES)

    pl.semaphore_wait(barrier, len(ring_peers) + len(side_peers) + len(rep_peers))

    def ids_copy(at):
        return pltpu.make_async_remote_copy(
            src_ref=ids_ref.at[at],
            dst_ref=heard.at[z],
            send_sem=ids_send.at[at],
            recv_sem=ids_recv.at[z],
            device_id=on_ring(at),
            device_id_type=MESH,
        )

    def ids_arrive(at):
        pltpu.make_async_copy(heard.at[at], heard.at[at], ids_recv.at[at]).wait()

    def start_ids(step, carry):
        ids_copy(plane(step)).start()
        return carry

    lax.fori_loop(1, count_z, start_ids, 0)

    def keep_copy(at):
        return pltpu.make_async_copy(heard.at[at], asked.at[at, side], ids_keep.at[at])

    def tell(at):
        keep_copy(at).start()
        for peer in side_peers:
            pltpu.make_async_remote_copy(
                src_ref=heard.at[at],
                dst_ref=asked.at[at, side],
                send_sem=ask_send.at[at],
                recv_sem=ask_recv.at[at],
                device_id=on_side(peer),
                device_id_type=MESH,
            ).start()

    def hear(step, carry=0):
        at = plane(step)
        ids_arrive(at)
        tell(at)
        return carry

    totals[...] = jnp.zeros_like(totals)
    tally[...] = jnp.zeros_like(tally)

    def look(step, carry=0):
        at = plane(step)
        keep_copy(at).wait()
        several = asked.at[at, pl.ds(0, count_s - 1)]
        pltpu.make_async_copy(several, several, ask_recv.at[at]).wait()
        shape = (count_s, slots, LANES)
        ids = jnp.broadcast_to(asked[at].astype(jnp.float32), shape)
        mine = lax.broadcasted_iota(jnp.int32, shape, 2) == side * slots + lax.broadcasted_iota(
            jnp.int32, shape, 1
        )
        wanted = jnp.sum(jnp.where(mine, ids, 0.0), axis=2, keepdims=True)
        wanted = jnp.broadcast_to(wanted, shape).reshape(count_s * slots, LANES)
        column[at] = wanted
        row_of = lax.broadcasted_iota(jnp.int32, wanted.shape, 1).astype(jnp.float32)
        hot = jnp.concatenate(
            [
                jnp.where(wanted == row_of + float(first), 1.0, 0.0).astype(jnp.bfloat16)
                for first in range(0, held, LANES)
            ],
            axis=1,
        )
        found = jnp.dot(hot, table[...], preferred_element_type=jnp.float32)
        found = found.reshape(count_s, slots, width)
        packed[at] = found.astype(jnp.bfloat16).reshape(count_x, count_c, slots, width)
        totals[...] += jnp.sum(found, axis=0)
        ones = jnp.ones((8, count_s * slots), jnp.bfloat16)
        tally[...] += jnp.dot(ones, hot, preferred_element_type=jnp.float32)
        return carry

    def row_copy(at):
        return pltpu.make_async_remote_copy(
            src_ref=packed.at[at],
            dst_ref=passing.at[z],
            send_sem=row_send.at[at],
            recv_sem=row_recv.at[z],
            device_id=on_ring(at),
            device_id_type=MESH,
        )

    def turn_keep_copy(at):
        return pltpu.make_async_copy(packed.at[at, x, c], turned.at[at, x, c], turn_keep.at[at])

    def turn(at):
        turn_keep_copy(at).start()
        for peer in side_peers:
            px, pc = lax.div(peer, count_c), lax.rem(peer, count_c)
            pltpu.make_async_remote_copy(
                src_ref=packed.at[at, px, pc],
                dst_ref=turned.at[at, x, c],
                send_sem=turn_send.at[at],
                recv_sem=turn_recv.at[at],
                device_id=on_side(peer),
                device_id_type=MESH,
            ).start()

    def pass_on(source, at):
        pltpu.make_async_copy(source.at[at, x, c], rows_ref.at[x, at, c], out_keep.at[at]).start()
        for peer in side_peers:
            px, pc = lax.div(peer, count_c), lax.rem(peer, count_c)
            pltpu.make_async_remote_copy(
                src_ref=source.at[at, px, pc],
                dst_ref=rows_ref.at[x, at, c],
                send_sem=out_send.at[at],
                recv_sem=out_recv.at[at],
                device_id=on_side(peer),
                device_id_type=MESH,
            ).start()

    def last_copy(at):
        return pltpu.make_async_remote_copy(
            src_ref=turned.at[at],
            dst_ref=rows_ref.at[:, z],
            send_sem=row_send.at[at],
            recv_sem=row_recv.at[z],
            device_id=on_ring(at),
            device_id_type=MESH,
        )

    def side_bytes(sem, at):
        several = passing.at[pl.ds(0, count_s - 1), 0, 0]
        pltpu.make_async_copy(several, several, sem.at[at]).wait()

    def last(step, carry=0):
        at = plane(step)
        turn_keep_copy(at).wait()
        side_bytes(turn_recv, at)
        last_copy(at).start()
        return carry

    relayed = min(6, (count_z - 3) // 2 * 2)
    early = min(3, count_z - 1 - relayed)

    def give(step, carry=0):
        at = plane(step)

        @pl.when(step == 0)
        def _():
            pass_on(packed, at)

        @pl.when((step >= 1) & (step <= relayed))
        def _():
            row_copy(at).start()

        @pl.when(step > relayed)
        def _():
            turn(at)

        return carry

    ahead = min(5, count_z - 2)
    heard[z] = ids_ref[z]
    tell(z)
    lax.fori_loop(1, ahead + 1, hear, 0)
    load_table.wait()

    def both(step, carry):
        look(step)
        hear(step + ahead + 1)
        give(step - 1)
        return carry

    def only(step, carry):
        look(step)
        give(step - 1)
        return carry

    look(0)
    hear(ahead + 1)
    lax.fori_loop(1, count_z - 1 - ahead, both, 0)
    lax.fori_loop(count_z - 1 - ahead, count_z, only, 0)

    tally_all[y] = tally[0:1].astype(jnp.int32)
    entries = jnp.sum(tally[0:1], axis=1, keepdims=True) * float(WIDTH)
    summed = jnp.sum(totals[...], axis=0, keepdims=True)
    means = [
        jnp.sum(summed[:, layer * WIDTH : (layer + 1) * WIDTH], axis=1, keepdims=True)
        / jnp.maximum(entries, 1.0)
        for layer in range(LAYERS)
    ]
    center = jnp.concatenate([jnp.broadcast_to(m, (1, WIDTH)) for m in means], axis=1)
    give(count_z - 1)

    def squares(at, total):
        used = column[at] >= 0.0
        used = jnp.concatenate([used.astype(jnp.float32)] * (width // LANES), axis=1)
        used = used.reshape(count_s, slots, width)
        rows = packed[at].reshape(count_s, slots, width).astype(jnp.float32)
        away = (rows - center[None]) * used
        return total + jnp.sum(away * away, axis=0)

    spread = lax.fori_loop(0, count_z, squares, jnp.zeros((slots, width), jnp.float32))
    spread = jnp.sum(spread, axis=0, keepdims=True)
    lane = lax.broadcasted_iota(jnp.int32, (1, LANES), 1)
    row = jnp.where(lane == 0, entries, 0.0)
    for layer in range(LAYERS):
        square = jnp.sum(spread[:, layer * WIDTH : (layer + 1) * WIDTH], axis=1, keepdims=True)
        row = jnp.where(lane == 1 + layer, means[layer], row)
        row = jnp.where(lane == 1 + LAYERS + layer, square, row)
    own_row[...] = row[None]
    parts_rep[y] = row

    def relay(step, carry=0):
        at = plane(step)
        pltpu.make_async_copy(passing.at[at], passing.at[at], row_recv.at[at]).wait()
        pass_on(passing, at)
        return carry

    for step in range(count_z - 1, count_z - 1 - early, -1):
        last(step)

    def tally_copy(peer):
        return pltpu.make_async_remote_copy(
            src_ref=tally_all.at[y],
            dst_ref=tally_all.at[y],
            send_sem=tally_send.at[peer],
            recv_sem=tally_recv.at[y],
            device_id=on_rep(peer),
            device_id_type=MESH,
        )

    def part_copy(source, parts, me, peer, place, send, recv):
        return pltpu.make_async_remote_copy(
            src_ref=source.at[0],
            dst_ref=parts.at[me],
            send_sem=send.at[peer],
            recv_sem=recv.at[me],
            device_id=place(peer),
            device_id_type=MESH,
        )

    def part_arrive(parts, peer, recv):
        pltpu.make_async_copy(parts.at[peer], parts.at[peer], recv.at[peer]).wait()

    def lanes_of(count):
        return lax.broadcasted_iota(jnp.int32, (count, 1, LANES), 2)

    for peer in rep_peers:
        part_copy(own_row, parts_rep, y, peer, on_rep, rep_send, rep_recv).start()
    for peer in rep_peers:
        tally_copy(peer).start()
    for peer in rep_peers:
        part_arrive(parts_rep, peer, rep_recv)
    side_row[...] = merged(parts_rep[...], lanes_of(count_y))
    parts_side[side] = side_row[0]
    for peer in rep_peers:
        pltpu.make_async_copy(tally_all.at[peer], tally_all.at[peer], tally_recv.at[peer]).wait()
    counts_ref[...] = jnp.sum(tally_all[...], axis=0)
    for peer in side_peers:
        part_copy(side_row, parts_side, side, peer, on_side, side_send, side_recv).start()
    for peer in side_peers:
        part_arrive(parts_side, peer, side_recv)
    plane_row[...] = merged(parts_side[...], lanes_of(count_s))
    parts_ring[z] = plane_row[0]
    relay(1)
    for peer in ring_peers:
        part_copy(plane_row, parts_ring, z, peer, on_ring, ring_send, ring_recv).start()
    for step in range(count_z - 1 - early, relayed, -1):
        last(step)
    lax.fori_loop(2, relayed + 1, relay, 0)
    for peer in ring_peers:
        part_arrive(parts_ring, peer, ring_recv)
    whole = merged(parts_ring[...], lanes_of(count_z))[0]

    def lone(at):
        return jnp.sum(jnp.where(lane == at, whole, 0.0), axis=1, keepdims=True)

    entries = lone(0)
    mean = [lone(1 + layer) for layer in range(LAYERS)]
    var = [lone(1 + LAYERS + layer) / entries for layer in range(LAYERS)]
    pair = lax.broadcasted_iota(jnp.int32, (1, LAYERS), 1)
    for row, values in enumerate((mean, var)):
        line = jnp.zeros((1, LAYERS), jnp.float32)
        for layer in range(LAYERS):
            line = jnp.where(pair == layer, values[layer], line)
        moments_ref[row : row + 1] = line
    for layer in range(LAYERS):
        span = slice(layer * WIDTH, (layer + 1) * WIDTH)
        affine_ref[0:1, span] = jnp.broadcast_to(mean[layer], (1, WIDTH))
        affine_ref[1:2, span] = lax.rsqrt(var[layer] + epsilon) * gain_ref[:, span]

    def finish(step, carry):
        at = plane(step)
        several_ids = asked.at[at, pl.ds(0, count_s - 1)]
        pltpu.make_async_copy(several_ids, several_ids, ask_send.at[at]).wait()

        @pl.when(step <= relayed)
        def _():
            side_bytes(out_send, at)
            side_bytes(out_recv, at)
            pltpu.make_async_copy(packed.at[at, x, c], rows_ref.at[x, at, c], out_keep.at[at]).wait()

        @pl.when(step > relayed)
        def _():
            side_bytes(turn_send, at)
            pltpu.make_async_copy(passing.at[at], passing.at[at], row_recv.at[at]).wait()

        return carry

    lax.fori_loop(0, count_z, finish, 0)

    def sent(step, carry):
        at = plane(step)
        ids_copy(at).wait_send()
        pltpu.make_async_copy(passing.at[at], passing.at[at], row_send.at[at]).wait()
        return carry

    lax.fori_loop(1, count_z, sent, 0)
    for peer in ring_peers:
        part_copy(plane_row, parts_ring, z, peer, on_ring, ring_send, ring_recv).wait_send()
    for peer in side_peers:
        part_copy(side_row, parts_side, side, peer, on_side, side_send, side_recv).wait_send()
    for peer in rep_peers:
        part_copy(own_row, parts_rep, y, peer, on_rep, rep_send, rep_recv).wait_send()
        tally_copy(peer).wait_send()


def finished(used_ref, rows_ref, affine_ref, tally_ref, moments_ref, out_ref, counts_ref, result_ref):
    block, slots, width = rows_ref.shape
    slot = lax.broadcasted_iota(jnp.int32, (slots, width), 0)
    mean = jnp.broadcast_to(affine_ref[0:1], (slots, width))
    scale = jnp.broadcast_to(affine_ref[1:2], (slots, width))
    first = pl.program_id(0) * block
    for at in range(block):
        value = (rows_ref[at].astype(jnp.float32) - mean) * scale
        value = jnp.where(slot < used_ref[0, first + at], value, 0.0)
        out_ref[at] = value.astype(jnp.bfloat16)
    counts_ref[...] = tally_ref[...]
    result_ref[...] = moments_ref[...]


def per_device(requests, request_counts, table, gain):
    sizes = tuple(lax.axis_size(axis) for axis in ROWS_REP)
    count_x, count_z, count_c, count_y = sizes
    count_s = count_x * count_c
    owners, slots = requests.shape[1:]
    held, width = table.shape

    dma = pltpu.SemaphoreType.DMA
    vmem = pltpu.VMEM
    rows, tally, moments, affine = pl.pallas_call(
        functools.partial(exchange, sizes, slots),
        out_shape=(
            jax.ShapeDtypeStruct((count_x, count_z, count_c, slots, width), jnp.bfloat16),
            jax.ShapeDtypeStruct((1, held), jnp.int32),
            jax.ShapeDtypeStruct((2, LAYERS), jnp.float32),
            jax.ShapeDtypeStruct((2, width), jnp.float32),
        ),
        in_specs=[
            pl.BlockSpec(memory_space=pltpu.VMEM),
            pl.BlockSpec(memory_space=pltpu.VMEM),
            pl.BlockSpec(memory_space=pltpu.VMEM),
            pl.BlockSpec(memory_space=pl.ANY),
        ],
        out_specs=(
            pl.BlockSpec(memory_space=pl.ANY),
            pl.BlockSpec(memory_space=pltpu.VMEM),
            pl.BlockSpec(memory_space=pltpu.VMEM),
            pl.BlockSpec(memory_space=pltpu.VMEM),
        ),
        scratch_shapes=[
            vmem((held, width), jnp.bfloat16),
            vmem((owners, LANES), jnp.int32),
            vmem((count_z, 1, LANES), jnp.int32),
            vmem((count_z, 1, LANES), jnp.int32),
            vmem((count_z, count_s, 1, LANES), jnp.int32),
            vmem((count_z, count_s * slots, LANES), jnp.float32),
            vmem((count_z, count_x, count_c, slots, width), jnp.bfloat16),
            vmem((count_z, count_x, count_c, slots, width), jnp.bfloat16),
            vmem((count_z, count_x, count_c, slots, width), jnp.bfloat16),
            vmem((slots, width), jnp.float32),
            vmem((8, held), jnp.float32),
            vmem((count_y, 1, held), jnp.int32),
            vmem((1, 1, LANES), jnp.float32),
            vmem((1, 1, LANES), jnp.float32),
            vmem((1, 1, LANES), jnp.float32),
            vmem((count_y, 1, LANES), jnp.float32),
            vmem((count_s, 1, LANES), jnp.float32),
            vmem((count_z, 1, LANES), jnp.float32),
            dma((1,)),
            dma((count_z,)),
            dma((count_z,)),
            dma((count_z,)),
            dma((count_z,)),
            dma((count_z,)),
            dma((count_z,)),
            dma((count_z,)),
            dma((count_z,)),
            dma((count_z,)),
            dma((count_z,)),
            dma((count_z,)),
            dma((count_z,)),
            dma((count_z,)),
            dma((count_y,)),
            dma((count_y,)),
            dma((count_y,)),
            dma((count_y,)),
            dma((count_s,)),
            dma((count_s,)),
            dma((count_z,)),
            dma((count_z,)),
        ],
        compiler_params=pltpu.CompilerParams(collective_id=0, has_side_effects=True),
    )(requests[0].T, request_counts, gain[None], table)

    steps = 4
    block = owners // steps
    rows, tally, moments = pl.pallas_call(
        finished,
        grid=(steps,),
        out_shape=(
            jax.ShapeDtypeStruct((owners, slots, width), jnp.bfloat16),
            jax.ShapeDtypeStruct((1, held), jnp.int32),
            jax.ShapeDtypeStruct((2, LAYERS), jnp.float32),
        ),
        in_specs=[
            pl.BlockSpec(memory_space=pltpu.SMEM),
            pl.BlockSpec((block, slots, width), lambda i: (i, 0, 0)),
            pl.BlockSpec((2, width), lambda i: (0, 0)),
            pl.BlockSpec((1, held), lambda i: (0, 0)),
            pl.BlockSpec((2, LAYERS), lambda i: (0, 0)),
        ],
        out_specs=(
            pl.BlockSpec((block, slots, width), lambda i: (i, 0, 0)),
            pl.BlockSpec((1, held), lambda i: (0, 0)),
            pl.BlockSpec((2, LAYERS), lambda i: (0, 0)),
        ),
    )(request_counts, rows.reshape(owners, slots, width), affine, tally, moments)
    return (rows[None], tally[0], moments)


def solution(mesh):
    count_y = mesh.shape["rep"]
    cores = 2
    count_x = mesh.devices.shape[0] // (16 * cores)
    finer = Mesh(mesh.devices.reshape(count_x, 16, cores, count_y), ROWS_REP)
    placed = (P(ROWS_REP, None, None), P(ROWS_REP, None), P(ROWS, None), P())
    return jax.shard_map(
        per_device,
        mesh=finer,
        in_specs=placed,
        out_specs=(P(ROWS_REP, None, None, None), P(ROWS), P()),
        check_vma=False,
    )
```

```python
import functools

import jax
import jax.numpy as jnp
from jax import lax
from jax.experimental import pallas as pl
from jax.experimental.pallas import tpu as pltpu
from jax.sharding import Mesh
from jax.sharding import PartitionSpec as P

WIDTH = 256
LAYERS = 2
LANES = 128
ROWS = ("rows_0", "rows_1", "rows_2")
ROWS_REP = ("rows_0", "rows_1", "rows_2", "rep")
MESH = pl.DeviceIdType.MESH
LATE = (3, 1)
BLOCKS = 4
KERNEL_BYTES = 20 * 2**20

epsilon = 1e-06


def merged(parts, lane):
    def pick(at):
        found = jnp.sum(jnp.where(lane == at, parts, 0.0), axis=2, keepdims=True)
        return jnp.broadcast_to(found, parts.shape)

    def over(value):
        return jnp.sum(value, axis=0, keepdims=True)

    line = lane[:1]
    each = pick(0)
    entries = over(each)
    row = jnp.where(line == 0, entries, 0.0)
    for layer in range(LAYERS):
        mean_each = pick(1 + layer)
        mean = over(each * mean_each) / jnp.maximum(entries, 1.0)
        gap = mean_each - mean
        square = over(pick(1 + LAYERS + layer) + each * gap * gap)
        row = jnp.where(line == 1 + layer, mean, row)
        row = jnp.where(line == 1 + LAYERS + layer, square, row)
    return row


def exchange(
    sizes,
    slots,
    requests_hbm,
    used_hbm,
    gain_hbm,
    table_ref,
    rows_ref,
    counts_ref,
    moments_ref,
    affine_ref,
    spread_ref,
    table,
    requests_ref,
    used_ref,
    gain_ref,
    upright,
    ids_ref,
    heard,
    asked,
    column,
    packed,
    passing,
    turned,
    totals,
    tally,
    tally_all,
    own_row,
    side_row,
    plane_row,
    parts_rep,
    parts_side,
    parts_ring,
    local_sem,
    ids_send,
    ids_recv,
    ids_keep,
    ask_send,
    ask_recv,
    row_send,
    row_recv,
    turn_send,
    turn_recv,
    turn_keep,
    out_send,
    out_recv,
    out_keep,
    tally_send,
    tally_recv,
    rep_send,
    rep_recv,
    side_send,
    side_recv,
    ring_send,
    ring_recv,
):
    count_x, count_z, count_c, count_y = sizes
    count_s = count_x * count_c
    held = table.shape[0]
    width = table.shape[1]
    x = lax.axis_index("rows_0")
    z = lax.axis_index("rows_1")
    c = lax.axis_index("rows_2")
    y = lax.axis_index("rep")
    side = x * count_c + c

    def on_ring(at):
        return {"rows_1": at}

    def on_side(at):
        return {"rows_0": lax.div(at, count_c), "rows_2": lax.rem(at, count_c)}

    def on_rep(at):
        return {"rep": at}

    ring_peers = [lax.rem(z + k, count_z) for k in range(1, count_z)]
    side_peers = [lax.rem(side + k, count_s) for k in range(1, count_s)]
    rep_peers = [lax.rem(y + k, count_y) for k in range(1, count_y)]

    def plane(step):
        far = lax.div(step + 1, 2)
        toward = 2 * lax.rem(step, 2) - 1
        return lax.rem(z + far * toward + count_z, count_z)

    loads = [
        pltpu.make_async_copy(source, target, local_sem.at[at])
        for at, (source, target) in enumerate(
            (
                (requests_hbm, requests_ref),
                (used_hbm, used_ref),
                (gain_hbm, gain_ref),
                (table_ref, table),
            )
        )
    ]
    for load in loads:
        load.start()
    load_table = loads.pop()

    barrier = pltpu.get_barrier_semaphore()
    for peer in ring_peers:
        pl.semaphore_signal(barrier, inc=1, device_id=on_ring(peer), device_id_type=MESH)
    for peer in side_peers:
        pl.semaphore_signal(barrier, inc=1, device_id=on_side(peer), device_id_type=MESH)
    for peer in rep_peers:
        pl.semaphore_signal(barrier, inc=1, device_id=on_rep(peer), device_id_type=MESH)

    for load in loads:
        load.wait()
    slot = lax.broadcasted_iota(jnp.int32, requests_ref.shape, 0)
    ids = jnp.where(slot < used_ref[...], requests_ref[...], -1)
    owners = ids.shape[1]
    ids = jnp.concatenate([ids, jnp.zeros((LANES - slots, owners), jnp.int32)], axis=0)
    upright[...] = jnp.transpose(ids)
    spread_ref[...] = jnp.transpose(jnp.broadcast_to(used_ref[...], (LANES, owners)))
    lines = jnp.zeros((count_z, LANES), jnp.int32)
    for at in range(count_s):
        first = (at // count_c) * count_z * count_c + at % count_c
        line = upright[pl.ds(first, count_z, stride=count_c), :]
        lines += pltpu.roll(line, slots * at, 1) if at else line
    ids_ref[...] = lines.reshape(count_z, 1, LANES)

    pl.semaphore_wait(barrier, len(ring_peers) + len(side_peers) + len(rep_peers))

    def ids_copy(at):
        return pltpu.make_async_remote_copy(
            src_ref=ids_ref.at[at],
            dst_ref=heard.at[z],
            send_sem=ids_send.at[at],
            recv_sem=ids_recv.at[z],
            device_id=on_ring(at),
            device_id_type=MESH,
        )

    def ids_arrive(at):
        pltpu.make_async_copy(heard.at[at], heard.at[at], ids_recv.at[at]).wait()

    def start_ids(step, carry):
        ids_copy(plane(step)).start()
        return carry

    lax.fori_loop(1, count_z, start_ids, 0)

    def keep_copy(at):
        return pltpu.make_async_copy(heard.at[at], asked.at[at, side], ids_keep.at[at])

    def tell(at):
        keep_copy(at).start()
        for peer in side_peers:
            pltpu.make_async_remote_copy(
                src_ref=heard.at[at],
                dst_ref=asked.at[at, side],
                send_sem=ask_send.at[at],
                recv_sem=ask_recv.at[at],
                device_id=on_side(peer),
                device_id_type=MESH,
            ).start()

    def hear(step, carry=0):
        at = plane(step)
        ids_arrive(at)
        tell(at)
        return carry

    totals[...] = jnp.zeros_like(totals)
    tally[...] = jnp.zeros_like(tally)

    def look(step, carry=0):
        at = plane(step)
        keep_copy(at).wait()
        several = asked.at[at, pl.ds(0, count_s - 1)]
        pltpu.make_async_copy(several, several, ask_recv.at[at]).wait()
        shape = (count_s, slots, LANES)
        ids = jnp.broadcast_to(asked[at].astype(jnp.float32), shape)
        mine = lax.broadcasted_iota(jnp.int32, shape, 2) == side * slots + lax.broadcasted_iota(
            jnp.int32, shape, 1
        )
        wanted = jnp.sum(jnp.where(mine, ids, 0.0), axis=2, keepdims=True)
        wanted = jnp.broadcast_to(wanted, shape).reshape(count_s * slots, LANES)
        column[at] = wanted
        row_of = lax.broadcasted_iota(jnp.int32, wanted.shape, 1).astype(jnp.float32)
        hot = jnp.concatenate(
            [
                jnp.where(wanted == row_of + float(first), 1.0, 0.0).astype(jnp.bfloat16)
                for first in range(0, held, LANES)
            ],
            axis=1,
        )
        found = jnp.dot(hot, table[...], preferred_element_type=jnp.float32)
        found = found.reshape(count_s, slots, width)
        packed[at] = found.astype(jnp.bfloat16).reshape(count_x, count_c, slots, width)
        totals[...] += jnp.sum(found, axis=0)
        ones = jnp.ones((8, count_s * slots), jnp.bfloat16)
        tally[...] += jnp.dot(ones, hot, preferred_element_type=jnp.float32)
        return carry

    def row_copy(at):
        return pltpu.make_async_remote_copy(
            src_ref=packed.at[at],
            dst_ref=passing.at[z],
            send_sem=row_send.at[at],
            recv_sem=row_recv.at[z],
            device_id=on_ring(at),
            device_id_type=MESH,
        )

    def turn_keep_copy(at):
        return pltpu.make_async_copy(packed.at[at, x, c], turned.at[at, x, c], turn_keep.at[at])

    def turn(at):
        turn_keep_copy(at).start()
        for peer in side_peers:
            px, pc = lax.div(peer, count_c), lax.rem(peer, count_c)
            pltpu.make_async_remote_copy(
                src_ref=packed.at[at, px, pc],
                dst_ref=turned.at[at, x, c],
                send_sem=turn_send.at[at],
                recv_sem=turn_recv.at[at],
                device_id=on_side(peer),
                device_id_type=MESH,
            ).start()

    def pass_on(source, at):
        pltpu.make_async_copy(source.at[at, x, c], rows_ref.at[x, at, c], out_keep.at[at]).start()
        for peer in side_peers:
            px, pc = lax.div(peer, count_c), lax.rem(peer, count_c)
            pltpu.make_async_remote_copy(
                src_ref=source.at[at, px, pc],
                dst_ref=rows_ref.at[x, at, c],
                send_sem=out_send.at[at],
                recv_sem=out_recv.at[at],
                device_id=on_side(peer),
                device_id_type=MESH,
            ).start()

    def last_copy(at):
        return pltpu.make_async_remote_copy(
            src_ref=turned.at[at],
            dst_ref=rows_ref.at[:, z],
            send_sem=row_send.at[at],
            recv_sem=row_recv.at[z],
            device_id=on_ring(at),
            device_id_type=MESH,
        )

    def side_bytes(sem, at):
        several = passing.at[pl.ds(0, count_s - 1), 0, 0]
        pltpu.make_async_copy(several, several, sem.at[at]).wait()

    def last(step, carry=0):
        at = plane(step)
        turn_keep_copy(at).wait()
        side_bytes(turn_recv, at)
        last_copy(at).start()
        return carry

    def is_late(step):
        far = lax.div(step + 1, 2)
        found = far == LATE[0]
        for distance in LATE[1:]:
            found = found | (far == distance)
        return found

    late_steps = [2 * far - side for far in LATE for side in (1, 0)]
    soon_steps = [step for step in range(1, count_z) if step not in late_steps]

    def give(step, carry=0):
        at = plane(step)

        @pl.when(step == 0)
        def _():
            pass_on(packed, at)

        @pl.when((step >= 1) & jnp.logical_not(is_late(step)))
        def _():
            row_copy(at).start()

        @pl.when(is_late(step))
        def _():
            turn(at)

        return carry

    ahead = min(5, count_z - 2)
    heard[z] = ids_ref[z]
    tell(z)
    lax.fori_loop(1, ahead + 1, hear, 0)
    load_table.wait()

    def both(step, carry):
        look(step)
        hear(step + ahead + 1)
        give(step - 1)
        return carry

    def only(step, carry):
        look(step)
        give(step - 1)
        return carry

    look(0)
    hear(ahead + 1)
    lax.fori_loop(1, count_z - 1 - ahead, both, 0)
    lax.fori_loop(count_z - 1 - ahead, count_z, only, 0)

    tally_all[y] = tally[0:1].astype(jnp.int32)
    entries = jnp.sum(tally[0:1], axis=1, keepdims=True) * float(WIDTH)
    summed = jnp.sum(totals[...], axis=0, keepdims=True)
    means = [
        jnp.sum(summed[:, layer * WIDTH : (layer + 1) * WIDTH], axis=1, keepdims=True)
        / jnp.maximum(entries, 1.0)
        for layer in range(LAYERS)
    ]
    center = jnp.concatenate([jnp.broadcast_to(m, (1, WIDTH)) for m in means], axis=1)
    give(count_z - 1)

    def squares(at, total):
        used = column[at] >= 0.0
        used = jnp.concatenate([used.astype(jnp.float32)] * (width // LANES), axis=1)
        used = used.reshape(count_s, slots, width)
        rows = packed[at].reshape(count_s, slots, width).astype(jnp.float32)
        away = (rows - center[None]) * used
        return total + jnp.sum(away * away, axis=0)

    spread = lax.fori_loop(0, count_z, squares, jnp.zeros((slots, width), jnp.float32))
    spread = jnp.sum(spread, axis=0, keepdims=True)
    lane = lax.broadcasted_iota(jnp.int32, (1, LANES), 1)
    row = jnp.where(lane == 0, entries, 0.0)
    for layer in range(LAYERS):
        square = jnp.sum(spread[:, layer * WIDTH : (layer + 1) * WIDTH], axis=1, keepdims=True)
        row = jnp.where(lane == 1 + layer, means[layer], row)
        row = jnp.where(lane == 1 + LAYERS + layer, square, row)
    own_row[...] = row[None]
    parts_rep[y] = row

    def relay(step, carry=0):
        at = plane(step)

        @pl.when(jnp.logical_not(is_late(step)))
        def _():
            relay_plane(at)

        return carry

    def relay_plane(at):
        pltpu.make_async_copy(passing.at[at], passing.at[at], row_recv.at[at]).wait()
        pass_on(passing, at)

    def tally_copy(peer):
        return pltpu.make_async_remote_copy(
            src_ref=tally_all.at[y],
            dst_ref=tally_all.at[y],
            send_sem=tally_send.at[peer],
            recv_sem=tally_recv.at[y],
            device_id=on_rep(peer),
            device_id_type=MESH,
        )

    def part_copy(source, parts, me, peer, place, send, recv):
        return pltpu.make_async_remote_copy(
            src_ref=source.at[0],
            dst_ref=parts.at[me],
            send_sem=send.at[peer],
            recv_sem=recv.at[me],
            device_id=place(peer),
            device_id_type=MESH,
        )

    def part_arrive(parts, peer, recv):
        pltpu.make_async_copy(parts.at[peer], parts.at[peer], recv.at[peer]).wait()

    def lanes_of(count):
        return lax.broadcasted_iota(jnp.int32, (count, 1, LANES), 2)

    for peer in rep_peers:
        part_copy(own_row, parts_rep, y, peer, on_rep, rep_send, rep_recv).start()
    for peer in rep_peers:
        tally_copy(peer).start()
    for peer in rep_peers:
        part_arrive(parts_rep, peer, rep_recv)
    side_row[...] = merged(parts_rep[...], lanes_of(count_y))
    parts_side[side] = side_row[0]
    for peer in rep_peers:
        pltpu.make_async_copy(tally_all.at[peer], tally_all.at[peer], tally_recv.at[peer]).wait()
    counts_ref[...] = jnp.sum(tally_all[...], axis=0)
    for peer in side_peers:
        part_copy(side_row, parts_side, side, peer, on_side, side_send, side_recv).start()
    for peer in side_peers:
        part_arrive(parts_side, peer, side_recv)
    plane_row[...] = merged(parts_side[...], lanes_of(count_s))
    parts_ring[z] = plane_row[0]
    relay_plane(plane(soon_steps[0]))
    for peer in ring_peers:
        part_copy(plane_row, parts_ring, z, peer, on_ring, ring_send, ring_recv).start()
    for step in late_steps:
        last(step)
    lax.fori_loop(soon_steps[0] + 1, count_z, relay, 0)
    for peer in ring_peers:
        part_arrive(parts_ring, peer, ring_recv)
    whole = merged(parts_ring[...], lanes_of(count_z))[0]

    def lone(at):
        return jnp.sum(jnp.where(lane == at, whole, 0.0), axis=1, keepdims=True)

    entries = lone(0)
    mean = [lone(1 + layer) for layer in range(LAYERS)]
    var = [lone(1 + LAYERS + layer) / entries for layer in range(LAYERS)]
    pair = lax.broadcasted_iota(jnp.int32, (1, LAYERS), 1)
    for row, values in enumerate((mean, var)):
        line = jnp.zeros((1, LAYERS), jnp.float32)
        for layer in range(LAYERS):
            line = jnp.where(pair == layer, values[layer], line)
        moments_ref[row : row + 1] = line
    for layer in range(LAYERS):
        span = slice(layer * WIDTH, (layer + 1) * WIDTH)
        affine_ref[0:1, span] = jnp.broadcast_to(mean[layer], (1, WIDTH))
        affine_ref[1:2, span] = lax.rsqrt(var[layer] + epsilon) * gain_ref[:, span]

    def finish(step, carry):
        at = plane(step)
        several_ids = asked.at[at, pl.ds(0, count_s - 1)]
        pltpu.make_async_copy(several_ids, several_ids, ask_send.at[at]).wait()

        @pl.when(jnp.logical_not(is_late(step)))
        def _():
            side_bytes(out_send, at)
            side_bytes(out_recv, at)
            pltpu.make_async_copy(packed.at[at, x, c], rows_ref.at[x, at, c], out_keep.at[at]).wait()

        @pl.when(is_late(step))
        def _():
            side_bytes(turn_send, at)
            pltpu.make_async_copy(passing.at[at], passing.at[at], row_recv.at[at]).wait()

        return carry

    lax.fori_loop(0, count_z, finish, 0)

    def sent(step, carry):
        at = plane(step)
        ids_copy(at).wait_send()
        pltpu.make_async_copy(passing.at[at], passing.at[at], row_send.at[at]).wait()
        return carry

    lax.fori_loop(1, count_z, sent, 0)
    for peer in ring_peers:
        part_copy(plane_row, parts_ring, z, peer, on_ring, ring_send, ring_recv).wait_send()
    for peer in side_peers:
        part_copy(side_row, parts_side, side, peer, on_side, side_send, side_recv).wait_send()
    for peer in rep_peers:
        part_copy(own_row, parts_rep, y, peer, on_rep, rep_send, rep_recv).wait_send()
        tally_copy(peer).wait_send()


def finished(spread_ref, rows_ref, affine_ref, tally_ref, moments_ref, out_hbm, counts_ref, result_ref, done, done_sem):
    owners, slots, width = rows_ref.shape
    block = owners // BLOCKS
    slot = lax.broadcasted_iota(jnp.int32, (slots, width), 0)
    mean = jnp.broadcast_to(affine_ref[0:1], (slots, width))
    scale = jnp.broadcast_to(affine_ref[1:2], (slots, width))

    def send(part):
        span = pl.ds(part * block, block)
        return pltpu.make_async_copy(done.at[span], out_hbm.at[span], done_sem.at[part])

    for part in range(BLOCKS):
        for at in range(part * block, (part + 1) * block):
            value = (rows_ref[at].astype(jnp.float32) - mean) * scale
            used = jnp.concatenate([spread_ref[at : at + 1]] * (width // LANES), axis=1)
            value = jnp.where(slot < used, value, 0.0)
            done[at] = value.astype(jnp.bfloat16)
        if part:
            send(part - 1).start()
    counts_ref[...] = tally_ref[...]
    result_ref[...] = moments_ref[...]
    send(BLOCKS - 1).start()
    for part in range(BLOCKS):
        send(part).wait()


def per_device(requests, request_counts, table, gain):
    sizes = tuple(lax.axis_size(axis) for axis in ROWS_REP)
    count_x, count_z, count_c, count_y = sizes
    count_s = count_x * count_c
    owners, slots = requests.shape[1:]
    held, width = table.shape

    dma = pltpu.SemaphoreType.DMA
    vmem = pltpu.VMEM
    rows, tally, moments, affine, spread = pl.pallas_call(
        functools.partial(exchange, sizes, slots),
        out_shape=(
            jax.ShapeDtypeStruct((count_x, count_z, count_c, slots, width), jnp.bfloat16),
            jax.ShapeDtypeStruct((1, held), jnp.int32),
            jax.ShapeDtypeStruct((2, LAYERS), jnp.float32),
            jax.ShapeDtypeStruct((2, width), jnp.float32),
            jax.ShapeDtypeStruct((owners, LANES), jnp.int32),
        ),
        in_specs=[pl.BlockSpec(memory_space=pltpu.HBM)] * 4,
        out_specs=(
            pl.BlockSpec(memory_space=pl.ANY),
            pl.BlockSpec(memory_space=pltpu.VMEM),
            pl.BlockSpec(memory_space=pltpu.VMEM),
            pl.BlockSpec(memory_space=pltpu.VMEM),
            pl.BlockSpec(memory_space=pltpu.VMEM),
        ),
        scratch_shapes=[
            vmem((held, width), jnp.bfloat16),
            vmem((slots, owners), jnp.int32),
            vmem((1, owners), jnp.int32),
            vmem((1, width), jnp.float32),
            vmem((owners, LANES), jnp.int32),
            vmem((count_z, 1, LANES), jnp.int32),
            vmem((count_z, 1, LANES), jnp.int32),
            vmem((count_z, count_s, 1, LANES), jnp.int32),
            vmem((count_z, count_s * slots, LANES), jnp.float32),
            vmem((count_z, count_x, count_c, slots, width), jnp.bfloat16),
            vmem((count_z, count_x, count_c, slots, width), jnp.bfloat16),
            vmem((count_z, count_x, count_c, slots, width), jnp.bfloat16),
            vmem((slots, width), jnp.float32),
            vmem((8, held), jnp.float32),
            vmem((count_y, 1, held), jnp.int32),
            vmem((1, 1, LANES), jnp.float32),
            vmem((1, 1, LANES), jnp.float32),
            vmem((1, 1, LANES), jnp.float32),
            vmem((count_y, 1, LANES), jnp.float32),
            vmem((count_s, 1, LANES), jnp.float32),
            vmem((count_z, 1, LANES), jnp.float32),
            dma((4,)),
            dma((count_z,)),
            dma((count_z,)),
            dma((count_z,)),
            dma((count_z,)),
            dma((count_z,)),
            dma((count_z,)),
            dma((count_z,)),
            dma((count_z,)),
            dma((count_z,)),
            dma((count_z,)),
            dma((count_z,)),
            dma((count_z,)),
            dma((count_z,)),
            dma((count_y,)),
            dma((count_y,)),
            dma((count_y,)),
            dma((count_y,)),
            dma((count_s,)),
            dma((count_s,)),
            dma((count_z,)),
            dma((count_z,)),
        ],
        compiler_params=pltpu.CompilerParams(
            collective_id=0, has_side_effects=True, vmem_limit_bytes=KERNEL_BYTES
        ),
    )(
        *[
            pltpu.with_memory_space_constraint(value, pltpu.HBM)
            for value in (requests[0].T, request_counts, gain[None], table)
        ]
    )

    rows, tally, moments = pl.pallas_call(
        finished,
        out_shape=(
            jax.ShapeDtypeStruct((owners, slots, width), jnp.bfloat16),
            jax.ShapeDtypeStruct((1, held), jnp.int32),
            jax.ShapeDtypeStruct((2, LAYERS), jnp.float32),
        ),
        in_specs=[pl.BlockSpec(memory_space=pltpu.VMEM)] * 5,
        out_specs=(
            pl.BlockSpec(memory_space=pltpu.HBM),
            pl.BlockSpec(memory_space=pltpu.VMEM),
            pl.BlockSpec(memory_space=pltpu.VMEM),
        ),
        scratch_shapes=[vmem((owners, slots, width), jnp.bfloat16), dma((BLOCKS,))],
        compiler_params=pltpu.CompilerParams(vmem_limit_bytes=KERNEL_BYTES),
    )(spread, rows.reshape(owners, slots, width), affine, tally, moments)
    return (rows[None], tally[0], moments)


def solution(mesh):
    count_y = mesh.shape["rep"]
    cores = 2
    count_x = mesh.devices.shape[0] // (16 * cores)
    finer = Mesh(mesh.devices.reshape(count_x, 16, cores, count_y), ROWS_REP)
    placed = (P(ROWS_REP, None, None), P(ROWS_REP, None), P(ROWS, None), P())
    return jax.shard_map(
        per_device,
        mesh=finer,
        in_specs=placed,
        out_specs=(P(ROWS_REP, None, None, None), P(ROWS), P()),
        check_vma=False,
    )
```

```python
import functools

import jax
import jax.numpy as jnp
from jax import lax
from jax.experimental import pallas as pl
from jax.experimental.pallas import tpu as pltpu
from jax.sharding import Mesh
from jax.sharding import PartitionSpec as P

WIDTH = 256
LAYERS = 2
LANES = 128
ROWS = ("rows_0", "rows_1", "rows_2")
ROWS_REP = ("rows_0", "rows_1", "rows_2", "rep")
MESH = pl.DeviceIdType.MESH
LATE = (6, 4)
BLOCKS = 4
KERNEL_BYTES = 20 * 2**20

epsilon = 1e-06


def merged(parts, lane):
    def pick(at):
        found = jnp.sum(jnp.where(lane == at, parts, 0.0), axis=2, keepdims=True)
        return jnp.broadcast_to(found, parts.shape)

    def over(value):
        return jnp.sum(value, axis=0, keepdims=True)

    line = lane[:1]
    each = pick(0)
    entries = over(each)
    row = jnp.where(line == 0, entries, 0.0)
    for layer in range(LAYERS):
        mean_each = pick(1 + layer)
        mean = over(each * mean_each) / jnp.maximum(entries, 1.0)
        gap = mean_each - mean
        square = over(pick(1 + LAYERS + layer) + each * gap * gap)
        row = jnp.where(line == 1 + layer, mean, row)
        row = jnp.where(line == 1 + LAYERS + layer, square, row)
    return row


def exchange(
    sizes,
    slots,
    requests_hbm,
    used_hbm,
    gain_hbm,
    table_ref,
    rows_ref,
    counts_ref,
    moments_ref,
    affine_ref,
    spread_ref,
    table,
    requests_ref,
    used_ref,
    gain_ref,
    upright,
    ids_ref,
    heard,
    asked,
    column,
    packed,
    passing,
    turned,
    totals,
    tally,
    tally_all,
    own_row,
    side_row,
    plane_row,
    parts_rep,
    parts_side,
    parts_ring,
    local_sem,
    ids_send,
    ids_recv,
    ids_keep,
    ask_send,
    ask_recv,
    row_send,
    row_recv,
    turn_send,
    turn_recv,
    turn_keep,
    out_send,
    out_recv,
    out_keep,
    tally_send,
    tally_recv,
    rep_send,
    rep_recv,
    side_send,
    side_recv,
    ring_send,
    ring_recv,
):
    count_x, count_z, count_c, count_y = sizes
    count_s = count_x * count_c
    held = table.shape[0]
    width = table.shape[1]
    x = lax.axis_index("rows_0")
    z = lax.axis_index("rows_1")
    c = lax.axis_index("rows_2")
    y = lax.axis_index("rep")
    side = x * count_c + c

    def on_ring(at):
        return {"rows_1": at}

    def on_side(at):
        return {"rows_0": lax.div(at, count_c), "rows_2": lax.rem(at, count_c)}

    def on_rep(at):
        return {"rep": at}

    ring_peers = [lax.rem(z + k, count_z) for k in range(1, count_z)]
    side_peers = [lax.rem(side + k, count_s) for k in range(1, count_s)]
    rep_peers = [lax.rem(y + k, count_y) for k in range(1, count_y)]

    def plane(step):
        far = lax.div(step + 1, 2)
        toward = 2 * lax.rem(step, 2) - 1
        return lax.rem(z + far * toward + count_z, count_z)

    loads = [
        pltpu.make_async_copy(source, target, local_sem.at[at])
        for at, (source, target) in enumerate(
            (
                (requests_hbm, requests_ref),
                (used_hbm, used_ref),
                (gain_hbm, gain_ref),
                (table_ref, table),
            )
        )
    ]
    for load in loads:
        load.start()
    load_table = loads.pop()

    barrier = pltpu.get_barrier_semaphore()
    for peer in ring_peers:
        pl.semaphore_signal(barrier, inc=1, device_id=on_ring(peer), device_id_type=MESH)
    for peer in side_peers:
        pl.semaphore_signal(barrier, inc=1, device_id=on_side(peer), device_id_type=MESH)
    for peer in rep_peers:
        pl.semaphore_signal(barrier, inc=1, device_id=on_rep(peer), device_id_type=MESH)

    for load in loads:
        load.wait()
    slot = lax.broadcasted_iota(jnp.int32, requests_ref.shape, 0)
    ids = jnp.where(slot < used_ref[...], requests_ref[...], -1)
    owners = ids.shape[1]
    ids = jnp.concatenate([ids, jnp.zeros((LANES - slots, owners), jnp.int32)], axis=0)
    upright[...] = jnp.transpose(ids)
    spread_ref[...] = jnp.transpose(jnp.broadcast_to(used_ref[...], (LANES, owners)))
    lines = jnp.zeros((count_z, LANES), jnp.int32)
    for at in range(count_s):
        first = (at // count_c) * count_z * count_c + at % count_c
        line = upright[pl.ds(first, count_z, stride=count_c), :]
        lines += pltpu.roll(line, slots * at, 1) if at else line
    ids_ref[...] = lines.reshape(count_z, 1, LANES)

    pl.semaphore_wait(barrier, len(ring_peers) + len(side_peers) + len(rep_peers))

    def ids_copy(at):
        return pltpu.make_async_remote_copy(
            src_ref=ids_ref.at[at],
            dst_ref=heard.at[z],
            send_sem=ids_send.at[at],
            recv_sem=ids_recv.at[z],
            device_id=on_ring(at),
            device_id_type=MESH,
        )

    def ids_arrive(at):
        pltpu.make_async_copy(heard.at[at], heard.at[at], ids_recv.at[at]).wait()

    def start_ids(step, carry):
        ids_copy(plane(count_z - step)).start()
        return carry

    lax.fori_loop(1, count_z, start_ids, 0)

    def keep_copy(at):
        return pltpu.make_async_copy(heard.at[at], asked.at[at, side], ids_keep.at[at])

    def tell(at):
        keep_copy(at).start()
        for peer in side_peers:
            pltpu.make_async_remote_copy(
                src_ref=heard.at[at],
                dst_ref=asked.at[at, side],
                send_sem=ask_send.at[at],
                recv_sem=ask_recv.at[at],
                device_id=on_side(peer),
                device_id_type=MESH,
            ).start()

    def hear(step, carry=0):
        at = plane(step)
        ids_arrive(at)
        tell(at)
        return carry

    totals[...] = jnp.zeros_like(totals)
    tally[...] = jnp.zeros_like(tally)

    def look(step, carry=0):
        at = plane(step)
        keep_copy(at).wait()
        several = asked.at[at, pl.ds(0, count_s - 1)]
        pltpu.make_async_copy(several, several, ask_recv.at[at]).wait()
        shape = (count_s, slots, LANES)
        ids = jnp.broadcast_to(asked[at].astype(jnp.float32), shape)
        mine = lax.broadcasted_iota(jnp.int32, shape, 2) == side * slots + lax.broadcasted_iota(
            jnp.int32, shape, 1
        )
        wanted = jnp.sum(jnp.where(mine, ids, 0.0), axis=2, keepdims=True)
        wanted = jnp.broadcast_to(wanted, shape).reshape(count_s * slots, LANES)
        column[at] = wanted
        row_of = lax.broadcasted_iota(jnp.int32, wanted.shape, 1).astype(jnp.float32)
        hot = jnp.concatenate(
            [
                jnp.where(wanted == row_of + float(first), 1.0, 0.0).astype(jnp.bfloat16)
                for first in range(0, held, LANES)
            ],
            axis=1,
        )
        found = jnp.dot(hot, table[...], preferred_element_type=jnp.float32)
        found = found.reshape(count_s, slots, width)
        packed[at] = found.astype(jnp.bfloat16).reshape(count_x, count_c, slots, width)
        totals[...] += jnp.sum(found, axis=0)
        ones = jnp.ones((8, count_s * slots), jnp.bfloat16)
        tally[...] += jnp.dot(ones, hot, preferred_element_type=jnp.float32)
        return carry

    def row_copy(at):
        return pltpu.make_async_remote_copy(
            src_ref=packed.at[at],
            dst_ref=passing.at[z],
            send_sem=row_send.at[at],
            recv_sem=row_recv.at[z],
            device_id=on_ring(at),
            device_id_type=MESH,
        )

    def turn_keep_copy(at):
        return pltpu.make_async_copy(packed.at[at, x, c], turned.at[at, x, c], turn_keep.at[at])

    def turn(at):
        turn_keep_copy(at).start()
        for peer in side_peers:
            px, pc = lax.div(peer, count_c), lax.rem(peer, count_c)
            pltpu.make_async_remote_copy(
                src_ref=packed.at[at, px, pc],
                dst_ref=turned.at[at, x, c],
                send_sem=turn_send.at[at],
                recv_sem=turn_recv.at[at],
                device_id=on_side(peer),
                device_id_type=MESH,
            ).start()

    def pass_on(source, at):
        pltpu.make_async_copy(source.at[at, x, c], rows_ref.at[x, at, c], out_keep.at[at]).start()
        for peer in side_peers:
            px, pc = lax.div(peer, count_c), lax.rem(peer, count_c)
            pltpu.make_async_remote_copy(
                src_ref=source.at[at, px, pc],
                dst_ref=rows_ref.at[x, at, c],
                send_sem=out_send.at[at],
                recv_sem=out_recv.at[at],
                device_id=on_side(peer),
                device_id_type=MESH,
            ).start()

    def last_copy(at):
        return pltpu.make_async_remote_copy(
            src_ref=turned.at[at],
            dst_ref=rows_ref.at[:, z],
            send_sem=row_send.at[at],
            recv_sem=row_recv.at[z],
            device_id=on_ring(at),
            device_id_type=MESH,
        )

    def side_bytes(sem, at):
        several = passing.at[pl.ds(0, count_s - 1), 0, 0]
        pltpu.make_async_copy(several, several, sem.at[at]).wait()

    def last(step, carry=0):
        at = plane(step)
        turn_keep_copy(at).wait()
        side_bytes(turn_recv, at)
        last_copy(at).start()
        return carry

    def is_late(step):
        far = lax.div(step + 1, 2)
        found = far == LATE[0]
        for distance in LATE[1:]:
            found = found | (far == distance)
        return found

    late_steps = [2 * far - side for far in LATE for side in (1, 0)]
    soon_steps = [step for step in range(1, count_z) if step not in late_steps]

    def give(step, carry=0):
        at = plane(step)

        @pl.when((step >= 1) & jnp.logical_not(is_late(step)))
        def _():
            row_copy(at).start()

        return carry

    ahead = min(5, count_z - 2)
    heard[z] = ids_ref[z]
    tell(z)
    lax.fori_loop(1, ahead + 1, hear, 0)
    load_table.wait()

    def both(step, carry):
        look(step)
        hear(step + ahead + 1)
        give(step - 1)
        return carry

    def only(step, carry):
        look(step)
        give(step - 1)
        return carry

    look(0)
    hear(ahead + 1)
    lax.fori_loop(1, count_z - 1 - ahead, both, 0)
    lax.fori_loop(count_z - 1 - ahead, count_z, only, 0)

    tally_all[y] = tally[0:1].astype(jnp.int32)
    entries = jnp.sum(tally[0:1], axis=1, keepdims=True) * float(WIDTH)
    summed = jnp.sum(totals[...], axis=0, keepdims=True)
    means = [
        jnp.sum(summed[:, layer * WIDTH : (layer + 1) * WIDTH], axis=1, keepdims=True)
        / jnp.maximum(entries, 1.0)
        for layer in range(LAYERS)
    ]
    center = jnp.concatenate([jnp.broadcast_to(m, (1, WIDTH)) for m in means], axis=1)
    give(count_z - 1)
    for step in late_steps:
        turn(plane(step))
    pass_on(packed, z)

    def squares(at, total):
        used = column[at] >= 0.0
        used = jnp.concatenate([used.astype(jnp.float32)] * (width // LANES), axis=1)
        used = used.reshape(count_s, slots, width)
        rows = packed[at].reshape(count_s, slots, width).astype(jnp.float32)
        away = (rows - center[None]) * used
        return total + jnp.sum(away * away, axis=0)

    spread = lax.fori_loop(0, count_z, squares, jnp.zeros((slots, width), jnp.float32))
    spread = jnp.sum(spread, axis=0, keepdims=True)
    lane = lax.broadcasted_iota(jnp.int32, (1, LANES), 1)
    row = jnp.where(lane == 0, entries, 0.0)
    for layer in range(LAYERS):
        square = jnp.sum(spread[:, layer * WIDTH : (layer + 1) * WIDTH], axis=1, keepdims=True)
        row = jnp.where(lane == 1 + layer, means[layer], row)
        row = jnp.where(lane == 1 + LAYERS + layer, square, row)
    own_row[...] = row[None]
    parts_rep[y] = row

    def relay(step, carry=0):
        at = plane(step)

        @pl.when(jnp.logical_not(is_late(step)))
        def _():
            relay_plane(at)

        return carry

    def relay_plane(at):
        pltpu.make_async_copy(passing.at[at], passing.at[at], row_recv.at[at]).wait()
        pass_on(passing, at)

    def tally_copy(peer):
        return pltpu.make_async_remote_copy(
            src_ref=tally_all.at[y],
            dst_ref=tally_all.at[y],
            send_sem=tally_send.at[peer],
            recv_sem=tally_recv.at[y],
            device_id=on_rep(peer),
            device_id_type=MESH,
        )

    def part_copy(source, parts, me, peer, place, send, recv):
        return pltpu.make_async_remote_copy(
            src_ref=source.at[0],
            dst_ref=parts.at[me],
            send_sem=send.at[peer],
            recv_sem=recv.at[me],
            device_id=place(peer),
            device_id_type=MESH,
        )

    def part_arrive(parts, peer, recv):
        pltpu.make_async_copy(parts.at[peer], parts.at[peer], recv.at[peer]).wait()

    def lanes_of(count):
        return lax.broadcasted_iota(jnp.int32, (count, 1, LANES), 2)

    for peer in rep_peers:
        part_copy(own_row, parts_rep, y, peer, on_rep, rep_send, rep_recv).start()
    for peer in rep_peers:
        tally_copy(peer).start()
    for peer in rep_peers:
        part_arrive(parts_rep, peer, rep_recv)
    side_row[...] = merged(parts_rep[...], lanes_of(count_y))
    parts_side[side] = side_row[0]
    for peer in rep_peers:
        pltpu.make_async_copy(tally_all.at[peer], tally_all.at[peer], tally_recv.at[peer]).wait()
    counts_ref[...] = jnp.sum(tally_all[...], axis=0)
    for peer in side_peers:
        part_copy(side_row, parts_side, side, peer, on_side, side_send, side_recv).start()
    for peer in side_peers:
        part_arrive(parts_side, peer, side_recv)
    plane_row[...] = merged(parts_side[...], lanes_of(count_s))
    parts_ring[z] = plane_row[0]
    relay_plane(plane(soon_steps[0]))
    for peer in ring_peers:
        part_copy(plane_row, parts_ring, z, peer, on_ring, ring_send, ring_recv).start()
    for step in late_steps:
        last(step)
    lax.fori_loop(soon_steps[0] + 1, count_z, relay, 0)
    for peer in ring_peers:
        part_arrive(parts_ring, peer, ring_recv)
    whole = merged(parts_ring[...], lanes_of(count_z))[0]

    def lone(at):
        return jnp.sum(jnp.where(lane == at, whole, 0.0), axis=1, keepdims=True)

    entries = lone(0)
    mean = [lone(1 + layer) for layer in range(LAYERS)]
    var = [lone(1 + LAYERS + layer) / entries for layer in range(LAYERS)]
    pair = lax.broadcasted_iota(jnp.int32, (1, LAYERS), 1)
    for row, values in enumerate((mean, var)):
        line = jnp.zeros((1, LAYERS), jnp.float32)
        for layer in range(LAYERS):
            line = jnp.where(pair == layer, values[layer], line)
        moments_ref[row : row + 1] = line
    for layer in range(LAYERS):
        span = slice(layer * WIDTH, (layer + 1) * WIDTH)
        affine_ref[0:1, span] = jnp.broadcast_to(mean[layer], (1, WIDTH))
        affine_ref[1:2, span] = lax.rsqrt(var[layer] + epsilon) * gain_ref[:, span]

    def finish(step, carry):
        at = plane(step)
        several_ids = asked.at[at, pl.ds(0, count_s - 1)]
        pltpu.make_async_copy(several_ids, several_ids, ask_send.at[at]).wait()

        @pl.when(jnp.logical_not(is_late(step)))
        def _():
            side_bytes(out_send, at)
            side_bytes(out_recv, at)
            pltpu.make_async_copy(packed.at[at, x, c], rows_ref.at[x, at, c], out_keep.at[at]).wait()

        @pl.when(is_late(step))
        def _():
            side_bytes(turn_send, at)
            pltpu.make_async_copy(passing.at[at], passing.at[at], row_recv.at[at]).wait()

        return carry

    lax.fori_loop(0, count_z, finish, 0)

    def sent(step, carry):
        at = plane(step)
        ids_copy(at).wait_send()
        pltpu.make_async_copy(passing.at[at], passing.at[at], row_send.at[at]).wait()
        return carry

    lax.fori_loop(1, count_z, sent, 0)
    for peer in ring_peers:
        part_copy(plane_row, parts_ring, z, peer, on_ring, ring_send, ring_recv).wait_send()
    for peer in side_peers:
        part_copy(side_row, parts_side, side, peer, on_side, side_send, side_recv).wait_send()
    for peer in rep_peers:
        part_copy(own_row, parts_rep, y, peer, on_rep, rep_send, rep_recv).wait_send()
        tally_copy(peer).wait_send()


def finished(spread_ref, rows_ref, affine_ref, tally_ref, moments_ref, out_hbm, counts_ref, result_ref, done, done_sem):
    owners, slots, width = rows_ref.shape
    block = owners // BLOCKS
    slot = lax.broadcasted_iota(jnp.int32, (slots, width), 0)
    mean = jnp.broadcast_to(affine_ref[0:1], (slots, width))
    scale = jnp.broadcast_to(affine_ref[1:2], (slots, width))

    def send(part):
        span = pl.ds(part * block, block)
        return pltpu.make_async_copy(done.at[span], out_hbm.at[span], done_sem.at[part])

    for part in range(BLOCKS):
        for at in range(part * block, (part + 1) * block):
            value = (rows_ref[at].astype(jnp.float32) - mean) * scale
            used = jnp.concatenate([spread_ref[at : at + 1]] * (width // LANES), axis=1)
            value = jnp.where(slot < used, value, 0.0)
            done[at] = value.astype(jnp.bfloat16)
        if part:
            send(part - 1).start()
    counts_ref[...] = tally_ref[...]
    result_ref[...] = moments_ref[...]
    send(BLOCKS - 1).start()
    for part in range(BLOCKS):
        send(part).wait()


def per_device(requests, request_counts, table, gain):
    sizes = tuple(lax.axis_size(axis) for axis in ROWS_REP)
    count_x, count_z, count_c, count_y = sizes
    count_s = count_x * count_c
    owners, slots = requests.shape[1:]
    held, width = table.shape

    dma = pltpu.SemaphoreType.DMA
    vmem = pltpu.VMEM
    rows, tally, moments, affine, spread = pl.pallas_call(
        functools.partial(exchange, sizes, slots),
        out_shape=(
            jax.ShapeDtypeStruct((count_x, count_z, count_c, slots, width), jnp.bfloat16),
            jax.ShapeDtypeStruct((1, held), jnp.int32),
            jax.ShapeDtypeStruct((2, LAYERS), jnp.float32),
            jax.ShapeDtypeStruct((2, width), jnp.float32),
            jax.ShapeDtypeStruct((owners, LANES), jnp.int32),
        ),
        in_specs=[pl.BlockSpec(memory_space=pltpu.HBM)] * 4,
        out_specs=(
            pl.BlockSpec(memory_space=pl.ANY),
            pl.BlockSpec(memory_space=pltpu.VMEM),
            pl.BlockSpec(memory_space=pltpu.VMEM),
            pl.BlockSpec(memory_space=pltpu.VMEM),
            pl.BlockSpec(memory_space=pltpu.VMEM),
        ),
        scratch_shapes=[
            vmem((held, width), jnp.bfloat16),
            vmem((slots, owners), jnp.int32),
            vmem((1, owners), jnp.int32),
            vmem((1, width), jnp.float32),
            vmem((owners, LANES), jnp.int32),
            vmem((count_z, 1, LANES), jnp.int32),
            vmem((count_z, 1, LANES), jnp.int32),
            vmem((count_z, count_s, 1, LANES), jnp.int32),
            vmem((count_z, count_s * slots, LANES), jnp.float32),
            vmem((count_z, count_x, count_c, slots, width), jnp.bfloat16),
            vmem((count_z, count_x, count_c, slots, width), jnp.bfloat16),
            vmem((count_z, count_x, count_c, slots, width), jnp.bfloat16),
            vmem((slots, width), jnp.float32),
            vmem((8, held), jnp.float32),
            vmem((count_y, 1, held), jnp.int32),
            vmem((1, 1, LANES), jnp.float32),
            vmem((1, 1, LANES), jnp.float32),
            vmem((1, 1, LANES), jnp.float32),
            vmem((count_y, 1, LANES), jnp.float32),
            vmem((count_s, 1, LANES), jnp.float32),
            vmem((count_z, 1, LANES), jnp.float32),
            dma((4,)),
            dma((count_z,)),
            dma((count_z,)),
            dma((count_z,)),
            dma((count_z,)),
            dma((count_z,)),
            dma((count_z,)),
            dma((count_z,)),
            dma((count_z,)),
            dma((count_z,)),
            dma((count_z,)),
            dma((count_z,)),
            dma((count_z,)),
            dma((count_z,)),
            dma((count_y,)),
            dma((count_y,)),
            dma((count_y,)),
            dma((count_y,)),
            dma((count_s,)),
            dma((count_s,)),
            dma((count_z,)),
            dma((count_z,)),
        ],
        compiler_params=pltpu.CompilerParams(
            collective_id=0, has_side_effects=True, vmem_limit_bytes=KERNEL_BYTES
        ),
    )(
        *[
            pltpu.with_memory_space_constraint(value, pltpu.HBM)
            for value in (requests[0].T, request_counts, gain[None], table)
        ]
    )

    rows, tally, moments = pl.pallas_call(
        finished,
        out_shape=(
            jax.ShapeDtypeStruct((owners, slots, width), jnp.bfloat16),
            jax.ShapeDtypeStruct((1, held), jnp.int32),
            jax.ShapeDtypeStruct((2, LAYERS), jnp.float32),
        ),
        in_specs=[pl.BlockSpec(memory_space=pltpu.VMEM)] * 5,
        out_specs=(
            pl.BlockSpec(memory_space=pltpu.HBM),
            pl.BlockSpec(memory_space=pltpu.VMEM),
            pl.BlockSpec(memory_space=pltpu.VMEM),
        ),
        scratch_shapes=[vmem((owners, slots, width), jnp.bfloat16), dma((BLOCKS,))],
        compiler_params=pltpu.CompilerParams(vmem_limit_bytes=KERNEL_BYTES),
    )(spread, rows.reshape(owners, slots, width), affine, tally, moments)
    return (rows[None], tally[0], moments)


def solution(mesh):
    count_y = mesh.shape["rep"]
    cores = 2
    count_x = mesh.devices.shape[0] // (16 * cores)
    finer = Mesh(mesh.devices.reshape(count_x, 16, cores, count_y), ROWS_REP)
    placed = (P(ROWS_REP, None, None), P(ROWS_REP, None), P(ROWS, None), P())
    return jax.shard_map(
        per_device,
        mesh=finer,
        in_specs=placed,
        out_specs=(P(ROWS_REP, None, None, None), P(ROWS), P()),
        check_vma=False,
    )
```

```python
import functools

import jax
import jax.numpy as jnp
from jax import lax
from jax.experimental import pallas as pl
from jax.experimental.pallas import tpu as pltpu
from jax.sharding import Mesh
from jax.sharding import PartitionSpec as P

WIDTH = 256
LAYERS = 2
LANES = 128
ROWS = ("rows_0", "rows_1", "rows_2")
ROWS_REP = ("rows_0", "rows_1", "rows_2", "rep")
MESH = pl.DeviceIdType.MESH
LATE = (6, 4)
BLOCKS = 4
KERNEL_BYTES = 20 * 2**20

epsilon = 1e-06


def merged(parts, lane):
    def pick(at):
        found = jnp.sum(jnp.where(lane == at, parts, 0.0), axis=2, keepdims=True)
        return jnp.broadcast_to(found, parts.shape)

    def over(value):
        return jnp.sum(value, axis=0, keepdims=True)

    line = lane[:1]
    each = pick(0)
    entries = over(each)
    row = jnp.where(line == 0, entries, 0.0)
    for layer in range(LAYERS):
        mean_each = pick(1 + layer)
        mean = over(each * mean_each) / jnp.maximum(entries, 1.0)
        gap = mean_each - mean
        square = over(pick(1 + LAYERS + layer) + each * gap * gap)
        row = jnp.where(line == 1 + layer, mean, row)
        row = jnp.where(line == 1 + LAYERS + layer, square, row)
    return row


def exchange(
    sizes,
    slots,
    requests_hbm,
    used_hbm,
    gain_hbm,
    table_ref,
    rows_ref,
    counts_ref,
    moments_ref,
    affine_ref,
    spread_ref,
    table,
    requests_ref,
    used_ref,
    gain_ref,
    upright,
    ids_ref,
    heard,
    asked,
    column,
    packed,
    passing,
    turned,
    totals,
    tally,
    tally_all,
    own_row,
    side_row,
    plane_row,
    parts_rep,
    parts_side,
    parts_ring,
    local_sem,
    ids_send,
    ids_recv,
    ids_keep,
    ask_send,
    ask_recv,
    row_send,
    row_recv,
    turn_send,
    turn_recv,
    turn_keep,
    out_send,
    out_recv,
    out_keep,
    tally_send,
    tally_recv,
    rep_send,
    rep_recv,
    side_send,
    side_recv,
    ring_send,
    ring_recv,
):
    count_x, count_z, count_c, count_y = sizes
    count_s = count_x * count_c
    held = table.shape[0]
    width = table.shape[1]
    x = lax.axis_index("rows_0")
    z = lax.axis_index("rows_1")
    c = lax.axis_index("rows_2")
    y = lax.axis_index("rep")
    side = x * count_c + c

    def on_ring(at):
        return {"rows_1": at}

    def on_side(at):
        return {"rows_0": lax.div(at, count_c), "rows_2": lax.rem(at, count_c)}

    def on_rep(at):
        return {"rep": at}

    ring_peers = [lax.rem(z + k, count_z) for k in range(1, count_z)]
    side_peers = [lax.rem(side + k, count_s) for k in range(1, count_s)]
    rep_peers = [lax.rem(y + k, count_y) for k in range(1, count_y)]

    def plane(step):
        far = lax.div(step + 1, 2)
        toward = 2 * lax.rem(step, 2) - 1
        return lax.rem(z + far * toward + count_z, count_z)

    loads = [
        pltpu.make_async_copy(source, target, local_sem.at[at])
        for at, (source, target) in enumerate(
            (
                (requests_hbm, requests_ref),
                (used_hbm, used_ref),
                (gain_hbm, gain_ref),
                (table_ref, table),
            )
        )
    ]
    for load in loads:
        load.start()
    load_table = loads.pop()

    barrier = pltpu.get_barrier_semaphore()
    for peer in ring_peers:
        pl.semaphore_signal(barrier, inc=1, device_id=on_ring(peer), device_id_type=MESH)
    for peer in side_peers:
        pl.semaphore_signal(barrier, inc=1, device_id=on_side(peer), device_id_type=MESH)
    for peer in rep_peers:
        pl.semaphore_signal(barrier, inc=1, device_id=on_rep(peer), device_id_type=MESH)

    for load in loads:
        load.wait()
    slot = lax.broadcasted_iota(jnp.int32, requests_ref.shape, 0)
    ids = jnp.where(slot < used_ref[...], requests_ref[...], -1)
    owners = ids.shape[1]
    ids = jnp.concatenate([ids, jnp.zeros((LANES - slots, owners), jnp.int32)], axis=0)
    upright[...] = jnp.transpose(ids)
    spread_ref[...] = jnp.transpose(jnp.broadcast_to(used_ref[...], (LANES, owners)))
    lines = jnp.zeros((count_z, LANES), jnp.int32)
    for at in range(count_s):
        first = (at // count_c) * count_z * count_c + at % count_c
        line = upright[pl.ds(first, count_z, stride=count_c), :]
        lines += pltpu.roll(line, slots * at, 1) if at else line
    ids_ref[...] = lines.reshape(count_z, 1, LANES)

    pl.semaphore_wait(barrier, len(ring_peers) + len(side_peers) + len(rep_peers))

    def ids_copy(at):
        return pltpu.make_async_remote_copy(
            src_ref=ids_ref.at[at],
            dst_ref=heard.at[z],
            send_sem=ids_send.at[at],
            recv_sem=ids_recv.at[z],
            device_id=on_ring(at),
            device_id_type=MESH,
        )

    def ids_arrive(at):
        pltpu.make_async_copy(heard.at[at], heard.at[at], ids_recv.at[at]).wait()

    def start_ids(step, carry):
        ids_copy(plane(count_z - step)).start()
        return carry

    lax.fori_loop(1, count_z, start_ids, 0)

    def keep_copy(at):
        return pltpu.make_async_copy(heard.at[at], asked.at[at, side], ids_keep.at[at])

    def tell(at):
        keep_copy(at).start()
        for peer in side_peers:
            pltpu.make_async_remote_copy(
                src_ref=heard.at[at],
                dst_ref=asked.at[at, side],
                send_sem=ask_send.at[at],
                recv_sem=ask_recv.at[at],
                device_id=on_side(peer),
                device_id_type=MESH,
            ).start()

    def hear(step, carry=0):
        at = plane(step)
        ids_arrive(at)
        tell(at)
        return carry

    totals[...] = jnp.zeros_like(totals)
    tally[...] = jnp.zeros_like(tally)

    def one_hot(wanted):
        row_of = lax.broadcasted_iota(jnp.int32, wanted.shape, 1).astype(jnp.float32)
        return jnp.concatenate(
            [
                jnp.where(wanted == row_of + float(first), 1.0, 0.0).astype(jnp.bfloat16)
                for first in range(0, held, LANES)
            ],
            axis=1,
        )

    def look(step, carry=0):
        at = plane(step)
        keep_copy(at).wait()
        several = asked.at[at, pl.ds(0, count_s - 1)]
        pltpu.make_async_copy(several, several, ask_recv.at[at]).wait()
        shape = (count_s, slots, LANES)
        ids = jnp.broadcast_to(asked[at].astype(jnp.float32), shape)
        mine = lax.broadcasted_iota(jnp.int32, shape, 2) == side * slots + lax.broadcasted_iota(
            jnp.int32, shape, 1
        )
        wanted = jnp.sum(jnp.where(mine, ids, 0.0), axis=2, keepdims=True)
        wanted = jnp.broadcast_to(wanted, shape).reshape(count_s * slots, LANES)
        column[at] = wanted
        hot = one_hot(wanted)
        found = jnp.dot(hot, table[...], preferred_element_type=jnp.float32)
        found = found.reshape(count_s, slots, width)
        packed[at] = found.astype(jnp.bfloat16).reshape(count_x, count_c, slots, width)
        return carry

    def row_copy(at):
        return pltpu.make_async_remote_copy(
            src_ref=packed.at[at],
            dst_ref=passing.at[z],
            send_sem=row_send.at[at],
            recv_sem=row_recv.at[z],
            device_id=on_ring(at),
            device_id_type=MESH,
        )

    def turn_keep_copy(at):
        return pltpu.make_async_copy(packed.at[at, x, c], turned.at[at, x, c], turn_keep.at[at])

    def turn(at):
        turn_keep_copy(at).start()
        for peer in side_peers:
            px, pc = lax.div(peer, count_c), lax.rem(peer, count_c)
            pltpu.make_async_remote_copy(
                src_ref=packed.at[at, px, pc],
                dst_ref=turned.at[at, x, c],
                send_sem=turn_send.at[at],
                recv_sem=turn_recv.at[at],
                device_id=on_side(peer),
                device_id_type=MESH,
            ).start()

    def pass_on(source, at):
        pltpu.make_async_copy(source.at[at, x, c], rows_ref.at[x, at, c], out_keep.at[at]).start()
        for peer in side_peers:
            px, pc = lax.div(peer, count_c), lax.rem(peer, count_c)
            pltpu.make_async_remote_copy(
                src_ref=source.at[at, px, pc],
                dst_ref=rows_ref.at[x, at, c],
                send_sem=out_send.at[at],
                recv_sem=out_recv.at[at],
                device_id=on_side(peer),
                device_id_type=MESH,
            ).start()

    def last_copy(at):
        return pltpu.make_async_remote_copy(
            src_ref=turned.at[at],
            dst_ref=rows_ref.at[:, z],
            send_sem=row_send.at[at],
            recv_sem=row_recv.at[z],
            device_id=on_ring(at),
            device_id_type=MESH,
        )

    def side_bytes(sem, at):
        several = passing.at[pl.ds(0, count_s - 1), 0, 0]
        pltpu.make_async_copy(several, several, sem.at[at]).wait()

    def last(step, carry=0):
        at = plane(step)
        turn_keep_copy(at).wait()
        side_bytes(turn_recv, at)
        last_copy(at).start()
        return carry

    def is_late(step):
        far = lax.div(step + 1, 2)
        found = far == LATE[0]
        for distance in LATE[1:]:
            found = found | (far == distance)
        return found

    late_steps = [2 * far - side for far in LATE for side in (1, 0)]
    soon_steps = [step for step in range(1, count_z) if step not in late_steps]

    def give(step, carry=0):
        at = plane(step)

        @pl.when((step >= 1) & jnp.logical_not(is_late(step)))
        def _():
            row_copy(at).start()

        return carry

    ahead = min(5, count_z - 2)
    heard[z] = ids_ref[z]
    tell(z)
    lax.fori_loop(1, ahead + 1, hear, 0)
    load_table.wait()

    def both(step, carry):
        look(step)
        hear(step + ahead + 1)
        give(step - 1)
        return carry

    def only(step, carry):
        look(step)
        give(step - 1)
        return carry

    look(0)
    hear(ahead + 1)
    lax.fori_loop(1, count_z - 1 - ahead, both, 0)
    lax.fori_loop(count_z - 1 - ahead, count_z, only, 0)

    for step in late_steps:
        turn(plane(step))
    give(count_z - 1)
    pass_on(packed, z)

    def count(at, carry):
        rows = packed[at].reshape(count_s, slots, width).astype(jnp.float32)
        totals[...] += jnp.sum(rows, axis=0)
        ones = jnp.ones((8, count_s * slots), jnp.bfloat16)
        tally[...] += jnp.dot(ones, one_hot(column[at]), preferred_element_type=jnp.float32)
        return carry

    lax.fori_loop(0, count_z, count, 0)
    tally_all[y] = tally[0:1].astype(jnp.int32)
    entries = jnp.sum(tally[0:1], axis=1, keepdims=True) * float(WIDTH)
    summed = jnp.sum(totals[...], axis=0, keepdims=True)
    means = [
        jnp.sum(summed[:, layer * WIDTH : (layer + 1) * WIDTH], axis=1, keepdims=True)
        / jnp.maximum(entries, 1.0)
        for layer in range(LAYERS)
    ]
    center = jnp.concatenate([jnp.broadcast_to(m, (1, WIDTH)) for m in means], axis=1)

    def squares(at, total):
        used = column[at] >= 0.0
        used = jnp.concatenate([used.astype(jnp.float32)] * (width // LANES), axis=1)
        used = used.reshape(count_s, slots, width)
        rows = packed[at].reshape(count_s, slots, width).astype(jnp.float32)
        away = (rows - center[None]) * used
        return total + jnp.sum(away * away, axis=0)

    spread = lax.fori_loop(0, count_z, squares, jnp.zeros((slots, width), jnp.float32))
    spread = jnp.sum(spread, axis=0, keepdims=True)
    lane = lax.broadcasted_iota(jnp.int32, (1, LANES), 1)
    row = jnp.where(lane == 0, entries, 0.0)
    for layer in range(LAYERS):
        square = jnp.sum(spread[:, layer * WIDTH : (layer + 1) * WIDTH], axis=1, keepdims=True)
        row = jnp.where(lane == 1 + layer, means[layer], row)
        row = jnp.where(lane == 1 + LAYERS + layer, square, row)
    own_row[...] = row[None]
    parts_rep[y] = row

    def relay(step, carry=0):
        at = plane(step)

        @pl.when(jnp.logical_not(is_late(step)))
        def _():
            relay_plane(at)

        return carry

    def relay_plane(at):
        pltpu.make_async_copy(passing.at[at], passing.at[at], row_recv.at[at]).wait()
        pass_on(passing, at)

    def tally_copy(peer):
        return pltpu.make_async_remote_copy(
            src_ref=tally_all.at[y],
            dst_ref=tally_all.at[y],
            send_sem=tally_send.at[peer],
            recv_sem=tally_recv.at[y],
            device_id=on_rep(peer),
            device_id_type=MESH,
        )

    def part_copy(source, parts, me, peer, place, send, recv):
        return pltpu.make_async_remote_copy(
            src_ref=source.at[0],
            dst_ref=parts.at[me],
            send_sem=send.at[peer],
            recv_sem=recv.at[me],
            device_id=place(peer),
            device_id_type=MESH,
        )

    def part_arrive(parts, peer, recv):
        pltpu.make_async_copy(parts.at[peer], parts.at[peer], recv.at[peer]).wait()

    def lanes_of(count):
        return lax.broadcasted_iota(jnp.int32, (count, 1, LANES), 2)

    for peer in rep_peers:
        part_copy(own_row, parts_rep, y, peer, on_rep, rep_send, rep_recv).start()
    for peer in rep_peers:
        tally_copy(peer).start()
    for peer in rep_peers:
        part_arrive(parts_rep, peer, rep_recv)
    side_row[...] = merged(parts_rep[...], lanes_of(count_y))
    parts_side[side] = side_row[0]
    for peer in rep_peers:
        pltpu.make_async_copy(tally_all.at[peer], tally_all.at[peer], tally_recv.at[peer]).wait()
    counts_ref[...] = jnp.sum(tally_all[...], axis=0)
    for peer in side_peers:
        part_copy(side_row, parts_side, side, peer, on_side, side_send, side_recv).start()
    for peer in side_peers:
        part_arrive(parts_side, peer, side_recv)
    plane_row[...] = merged(parts_side[...], lanes_of(count_s))
    parts_ring[z] = plane_row[0]
    relay_plane(plane(soon_steps[0]))
    for peer in ring_peers:
        part_copy(plane_row, parts_ring, z, peer, on_ring, ring_send, ring_recv).start()
    for step in late_steps:
        last(step)
    lax.fori_loop(soon_steps[0] + 1, count_z, relay, 0)
    for peer in ring_peers:
        part_arrive(parts_ring, peer, ring_recv)
    whole = merged(parts_ring[...], lanes_of(count_z))[0]

    def lone(at):
        return jnp.sum(jnp.where(lane == at, whole, 0.0), axis=1, keepdims=True)

    entries = lone(0)
    mean = [lone(1 + layer) for layer in range(LAYERS)]
    var = [lone(1 + LAYERS + layer) / entries for layer in range(LAYERS)]
    pair = lax.broadcasted_iota(jnp.int32, (1, LAYERS), 1)
    for row, values in enumerate((mean, var)):
        line = jnp.zeros((1, LAYERS), jnp.float32)
        for layer in range(LAYERS):
            line = jnp.where(pair == layer, values[layer], line)
        moments_ref[row : row + 1] = line
    for layer in range(LAYERS):
        span = slice(layer * WIDTH, (layer + 1) * WIDTH)
        affine_ref[0:1, span] = jnp.broadcast_to(mean[layer], (1, WIDTH))
        affine_ref[1:2, span] = lax.rsqrt(var[layer] + epsilon) * gain_ref[:, span]

    def finish(step, carry):
        at = plane(step)
        several_ids = asked.at[at, pl.ds(0, count_s - 1)]
        pltpu.make_async_copy(several_ids, several_ids, ask_send.at[at]).wait()

        @pl.when(jnp.logical_not(is_late(step)))
        def _():
            side_bytes(out_send, at)
            side_bytes(out_recv, at)
            pltpu.make_async_copy(packed.at[at, x, c], rows_ref.at[x, at, c], out_keep.at[at]).wait()

        @pl.when(is_late(step))
        def _():
            side_bytes(turn_send, at)
            pltpu.make_async_copy(passing.at[at], passing.at[at], row_recv.at[at]).wait()

        return carry

    lax.fori_loop(0, count_z, finish, 0)

    def sent(step, carry):
        at = plane(step)
        ids_copy(at).wait_send()
        pltpu.make_async_copy(passing.at[at], passing.at[at], row_send.at[at]).wait()
        return carry

    lax.fori_loop(1, count_z, sent, 0)
    for peer in ring_peers:
        part_copy(plane_row, parts_ring, z, peer, on_ring, ring_send, ring_recv).wait_send()
    for peer in side_peers:
        part_copy(side_row, parts_side, side, peer, on_side, side_send, side_recv).wait_send()
    for peer in rep_peers:
        part_copy(own_row, parts_rep, y, peer, on_rep, rep_send, rep_recv).wait_send()
        tally_copy(peer).wait_send()


def finished(spread_ref, rows_ref, affine_ref, tally_ref, moments_ref, out_hbm, counts_ref, result_ref, done, done_sem):
    owners, slots, width = rows_ref.shape
    block = owners // BLOCKS
    slot = lax.broadcasted_iota(jnp.int32, (slots, width), 0)
    mean = jnp.broadcast_to(affine_ref[0:1], (slots, width))
    scale = jnp.broadcast_to(affine_ref[1:2], (slots, width))

    def send(part):
        span = pl.ds(part * block, block)
        return pltpu.make_async_copy(done.at[span], out_hbm.at[span], done_sem.at[part])

    for part in range(BLOCKS):
        for at in range(part * block, (part + 1) * block):
            value = (rows_ref[at].astype(jnp.float32) - mean) * scale
            used = jnp.concatenate([spread_ref[at : at + 1]] * (width // LANES), axis=1)
            value = jnp.where(slot < used, value, 0.0)
            done[at] = value.astype(jnp.bfloat16)
        if part:
            send(part - 1).start()
    counts_ref[...] = tally_ref[...]
    result_ref[...] = moments_ref[...]
    send(BLOCKS - 1).start()
    for part in range(BLOCKS):
        send(part).wait()


def per_device(requests, request_counts, table, gain):
    sizes = tuple(lax.axis_size(axis) for axis in ROWS_REP)
    count_x, count_z, count_c, count_y = sizes
    count_s = count_x * count_c
    owners, slots = requests.shape[1:]
    held, width = table.shape

    dma = pltpu.SemaphoreType.DMA
    vmem = pltpu.VMEM
    rows, tally, moments, affine, spread = pl.pallas_call(
        functools.partial(exchange, sizes, slots),
        out_shape=(
            jax.ShapeDtypeStruct((count_x, count_z, count_c, slots, width), jnp.bfloat16),
            jax.ShapeDtypeStruct((1, held), jnp.int32),
            jax.ShapeDtypeStruct((2, LAYERS), jnp.float32),
            jax.ShapeDtypeStruct((2, width), jnp.float32),
            jax.ShapeDtypeStruct((owners, LANES), jnp.int32),
        ),
        in_specs=[pl.BlockSpec(memory_space=pltpu.HBM)] * 4,
        out_specs=(
            pl.BlockSpec(memory_space=pl.ANY),
            pl.BlockSpec(memory_space=pltpu.VMEM),
            pl.BlockSpec(memory_space=pltpu.VMEM),
            pl.BlockSpec(memory_space=pltpu.VMEM),
            pl.BlockSpec(memory_space=pltpu.VMEM),
        ),
        scratch_shapes=[
            vmem((held, width), jnp.bfloat16),
            vmem((slots, owners), jnp.int32),
            vmem((1, owners), jnp.int32),
            vmem((1, width), jnp.float32),
            vmem((owners, LANES), jnp.int32),
            vmem((count_z, 1, LANES), jnp.int32),
            vmem((count_z, 1, LANES), jnp.int32),
            vmem((count_z, count_s, 1, LANES), jnp.int32),
            vmem((count_z, count_s * slots, LANES), jnp.float32),
            vmem((count_z, count_x, count_c, slots, width), jnp.bfloat16),
            vmem((count_z, count_x, count_c, slots, width), jnp.bfloat16),
            vmem((count_z, count_x, count_c, slots, width), jnp.bfloat16),
            vmem((slots, width), jnp.float32),
            vmem((8, held), jnp.float32),
            vmem((count_y, 1, held), jnp.int32),
            vmem((1, 1, LANES), jnp.float32),
            vmem((1, 1, LANES), jnp.float32),
            vmem((1, 1, LANES), jnp.float32),
            vmem((count_y, 1, LANES), jnp.float32),
            vmem((count_s, 1, LANES), jnp.float32),
            vmem((count_z, 1, LANES), jnp.float32),
            dma((4,)),
            dma((count_z,)),
            dma((count_z,)),
            dma((count_z,)),
            dma((count_z,)),
            dma((count_z,)),
            dma((count_z,)),
            dma((count_z,)),
            dma((count_z,)),
            dma((count_z,)),
            dma((count_z,)),
            dma((count_z,)),
            dma((count_z,)),
            dma((count_z,)),
            dma((count_y,)),
            dma((count_y,)),
            dma((count_y,)),
            dma((count_y,)),
            dma((count_s,)),
            dma((count_s,)),
            dma((count_z,)),
            dma((count_z,)),
        ],
        compiler_params=pltpu.CompilerParams(
            collective_id=0, has_side_effects=True, vmem_limit_bytes=KERNEL_BYTES
        ),
    )(
        *[
            pltpu.with_memory_space_constraint(value, pltpu.HBM)
            for value in (requests[0].T, request_counts, gain[None], table)
        ]
    )

    rows, tally, moments = pl.pallas_call(
        finished,
        out_shape=(
            jax.ShapeDtypeStruct((owners, slots, width), jnp.bfloat16),
            jax.ShapeDtypeStruct((1, held), jnp.int32),
            jax.ShapeDtypeStruct((2, LAYERS), jnp.float32),
        ),
        in_specs=[pl.BlockSpec(memory_space=pltpu.VMEM)] * 5,
        out_specs=(
            pl.BlockSpec(memory_space=pltpu.HBM),
            pl.BlockSpec(memory_space=pltpu.VMEM),
            pl.BlockSpec(memory_space=pltpu.VMEM),
        ),
        scratch_shapes=[vmem((owners, slots, width), jnp.bfloat16), dma((BLOCKS,))],
        compiler_params=pltpu.CompilerParams(vmem_limit_bytes=KERNEL_BYTES),
    )(spread, rows.reshape(owners, slots, width), affine, tally, moments)
    return (rows[None], tally[0], moments)


def solution(mesh):
    count_y = mesh.shape["rep"]
    cores = 2
    count_x = mesh.devices.shape[0] // (16 * cores)
    finer = Mesh(mesh.devices.reshape(count_x, 16, cores, count_y), ROWS_REP)
    placed = (P(ROWS_REP, None, None), P(ROWS_REP, None), P(ROWS, None), P())
    return jax.shard_map(
        per_device,
        mesh=finer,
        in_specs=placed,
        out_specs=(P(ROWS_REP, None, None, None), P(ROWS), P()),
        check_vma=False,
    )
```
